8 devices in a mesh: rep: 2 (over z, y), grp: 4 (over x, core).
Axes of the slice: x: 2, y: 2, z: 1, core: 2. Of those that a mesh axis runs over, the one named last changes fastest.
Arguments:
- x_in: bfloat16 [512, 3584], P(('rep', 'grp')), parts along dimension 0
- seq_len: int32 [512], P(('rep', 'grp')), parts along dimension 0
- k_cache: bfloat16 [512, 256, 4, 128], P(('rep', 'grp')), parts along dimension 0
- v_cache: bfloat16 [512, 256, 4, 128], P(('rep', 'grp')), parts along dimension 0
- gamma_attn: bfloat16 [3584], replicated
- w_qkv: bfloat16 [3584, 4608], replicated
- b_qkv: bfloat16 [4608], replicated
- w_proj: bfloat16 [3584, 3584], replicated
- gamma_mlp: bfloat16 [3584], replicated
- w_in: bfloat16 [2, 18944, 3584], P(None, 'grp')
- w_out: bfloat16 [18944, 3584], P('grp')
Outputs:
- output 1: bfloat16 [512, 3584], P(('rep', 'grp')), parts along dimension 0
- output 2: bfloat16 [512, 256, 4, 128], P(('rep', 'grp')), parts along dimension 0
- output 3: bfloat16 [512, 256, 4, 128], P(('rep', 'grp')), parts along dimension 0
There are 2 independent parts. The reference program is written for one: setup_inputs(seed, part) draws one part's arguments, and reference() takes and returns one part's arrays. A program takes and returns all parts, laid end to end along the dimension named above; an argument that names none is the same for every part.
All inputs are finite; a program needn't handle non-finite values.
Results may differ from the reference program's by a relative error of at most 0.00754008.
Values are sent between devices in bfloat16 or wider.
A program may use at most 1 GiB of HBM per device.

```python
import jax
import jax.numpy as jnp
from jax import lax

HIDDEN = 3584
HEADS = 28
KV_HEADS = 4
HEAD = 128
FFN = 18944
LMAX = 256
BATCH = 256
ROPE_BASE = 10000
QKV_WIDTH = (HEADS + 2 * KV_HEADS) * HEAD
ROT_DIM = HEAD // 2
EPS = 1e-5


def setup_inputs(seed: int = 0, part: int = 0) -> dict:
    keys = jax.random.split(jax.random.key(seed), 10)
    gamma_attn = (1.0 + 0.3 * jax.random.normal(keys[0], (HIDDEN,), jnp.float32)).astype(jnp.bfloat16)
    w_qkv = (jax.random.normal(keys[1], (HIDDEN, QKV_WIDTH), jnp.float32) * HIDDEN ** -0.5).astype(jnp.bfloat16)
    b_qkv = (0.5 * jax.random.normal(keys[2], (QKV_WIDTH,), jnp.float32)).astype(jnp.bfloat16)
    w_proj = (jax.random.normal(keys[3], (HEADS * HEAD, HIDDEN), jnp.float32) * (HEADS * HEAD) ** -0.5).astype(jnp.bfloat16)
    gamma_mlp = (1.0 + 0.3 * jax.random.normal(keys[4], (HIDDEN,), jnp.float32)).astype(jnp.bfloat16)
    w_in = (jax.random.normal(keys[5], (2, FFN, HIDDEN), jnp.float32) * HIDDEN ** -0.5).astype(jnp.bfloat16)
    w_out = (jax.random.normal(keys[6], (FFN, HIDDEN), jnp.float32) * FFN ** -0.5).astype(jnp.bfloat16)
    x_in = jax.random.normal(jax.random.fold_in(keys[7], part), (BATCH, HIDDEN), jnp.float32).astype(jnp.bfloat16)
    seq_len = jax.random.randint(jax.random.fold_in(keys[8], part), (BATCH,), 1, LMAX, dtype=jnp.int32)
    seq_len = seq_len.at[0].set(LMAX - 1).at[BATCH - 1].set(1)
    cache_keys = jax.random.split(jax.random.fold_in(keys[9], part), 3)
    cache_shape = (BATCH, LMAX, KV_HEADS, HEAD)
    k_cache = (2.0 * jax.random.normal(cache_keys[0], cache_shape, jnp.float32)).astype(jnp.bfloat16)
    drift = jnp.cumsum(jax.random.normal(cache_keys[1], cache_shape, jnp.float32), axis=1) * LMAX ** -0.5
    v_cache = (drift + jax.random.normal(cache_keys[2], cache_shape, jnp.float32)).astype(jnp.bfloat16)
    return {'x_in': x_in, 'seq_len': seq_len, 'k_cache': k_cache, 'v_cache': v_cache,
            'gamma_attn': gamma_attn, 'w_qkv': w_qkv, 'b_qkv': b_qkv, 'w_proj': w_proj,
            'gamma_mlp': gamma_mlp, 'w_in': w_in, 'w_out': w_out}


def rms_norm(vals, gain):
    mean_sq = jnp.mean(vals * vals, axis=-1, keepdims=True)
    return (vals * lax.rsqrt(mean_sq + EPS) * gain.astype(jnp.float32)).astype(jnp.bfloat16)


def rotary(vals, positions):
    inv_freq = ROPE_BASE ** (-jnp.arange(0, ROT_DIM, 2, dtype=jnp.float32) / ROT_DIM)
    angles = positions.astype(jnp.float32)[:, None] * inv_freq[None, :]
    cosine = jnp.cos(angles)[:, None, :]
    sine = jnp.sin(angles)[:, None, :]
    pairs = vals[..., :ROT_DIM].reshape(vals.shape[:-1] + (ROT_DIM // 2, 2))
    even_part = pairs[..., 0]
    odd_part = pairs[..., 1]
    rotated = jnp.stack([even_part * cosine - odd_part * sine, odd_part * cosine + even_part * sine], axis=-1)
    return jnp.concatenate([rotated.reshape(vals.shape[:-1] + (ROT_DIM,)), vals[..., ROT_DIM:]], axis=-1)


def reference(x_in, seq_len, k_cache, v_cache, gamma_attn, w_qkv, b_qkv, w_proj, gamma_mlp, w_in, w_out):
    x_f32 = x_in.astype(jnp.float32)
    normed = rms_norm(x_f32, gamma_attn)
    qkv_proj = jnp.dot(normed, w_qkv, preferred_element_type=jnp.float32) + b_qkv.astype(jnp.float32)
    q_width = HEADS * HEAD
    kv_width = KV_HEADS * HEAD
    query_rot = rotary(qkv_proj[:, :q_width].reshape(BATCH, HEADS, HEAD), seq_len).astype(jnp.bfloat16)
    key_new = rotary(qkv_proj[:, q_width:q_width + kv_width].reshape(BATCH, KV_HEADS, HEAD), seq_len).astype(jnp.bfloat16)
    value_new = qkv_proj[:, q_width + kv_width:].reshape(BATCH, KV_HEADS, HEAD).astype(jnp.bfloat16)
    positions = jnp.arange(LMAX, dtype=jnp.int32)
    at_len = (positions[None, :] == seq_len[:, None])[:, :, None, None]
    k_out = jnp.where(at_len, key_new[:, None], k_cache)
    v_out = jnp.where(at_len, value_new[:, None], v_cache)

    def one_seq(seq_args):
        q_row, k_row, v_row, length = seq_args
        q_grouped = q_row.reshape(KV_HEADS, HEADS // KV_HEADS, HEAD).astype(jnp.float32)
        attn_scores = jnp.einsum('gqd,lgd->gql', q_grouped, k_row.astype(jnp.float32)) * HEAD ** -0.5
        attn_scores = jnp.where((positions <= length)[None, None, :], attn_scores, -jnp.inf)
        attn_probs = jax.nn.softmax(attn_scores, axis=-1).astype(jnp.bfloat16)
        context = jnp.einsum('gql,lgd->gqd', attn_probs.astype(jnp.float32), v_row.astype(jnp.float32))
        return context.reshape(HEADS * HEAD).astype(jnp.bfloat16)

    context = lax.map(one_seq, (query_rot, k_out, v_out, seq_len))
    hidden = x_f32 + jnp.dot(context, w_proj, preferred_element_type=jnp.float32)
    mlp_in = rms_norm(hidden, gamma_mlp)
    gate_up = jnp.dot(mlp_in, w_in.reshape(2 * FFN, HIDDEN).T, preferred_element_type=jnp.float32)
    swiglu = (jax.nn.silu(gate_up[:, :FFN]) * gate_up[:, FFN:]).astype(jnp.bfloat16)
    mlp_out = jnp.dot(swiglu, w_out, preferred_element_type=jnp.float32)
    layer_out = (hidden + mlp_out).astype(jnp.bfloat16)
    return (layer_out, k_out, v_out)
```

```python
import functools

import jax
import jax.numpy as jnp
from jax import lax
from jax.experimental import pallas as pl
from jax.experimental.pallas import tpu as pltpu
from jax.sharding import PartitionSpec as P

HEAD = 128
ROPE_BASE = 10000.0
EPS = 1e-5
MESH = pl.DeviceIdType.MESH
F32 = jnp.float32
BF16 = jnp.bfloat16
LOG2E = 1.4426950408889634

QKV_COLS = 512
QKV_SLOTS = 4
SEQ_STEP = 4
SEQ_SLOTS = 4
HEAD_ROWS = 32
FF_BLOCK = 256
FF_SLOTS = 7
OUT_COLS = 512
OUT_SLOTS = 5
AG_CHUNKS = 4


def rms_norm(vals, gain):
    mean_sq = jnp.mean(vals * vals, axis=-1, keepdims=True)
    return (vals * lax.rsqrt(mean_sq + EPS) * gain.astype(F32)).astype(BF16)


def qkv_attention_kernel(q_heads, kv_heads, len_ref, x_ref, gain_ref, bias_ref, cos_ref, sin_ref, w_hbm, k_hbm, v_hbm,
                         ctx_ref, ko_hbm, vo_hbm, wbuf, kbuf, vbuf, n_scr, q_scr, kn_scr, vn_scr,
                         w_sem, ki_sem, vi_sem, ko_sem, vo_sem):
    rows = x_ref.shape[0]
    blocks = w_hbm.shape[1] // QKV_COLS
    steps = rows // SEQ_STEP
    group = q_heads // kv_heads
    heads_per_block = QKV_COLS // HEAD

    def w_copy(i):
        return pltpu.make_async_copy(w_hbm.at[:, pl.ds(i * QKV_COLS, QKV_COLS)], wbuf.at[i % QKV_SLOTS],
                                     w_sem.at[i % QKV_SLOTS])

    def in_copies(i):
        slot = lax.rem(i, SEQ_SLOTS)
        part = pl.ds(i * SEQ_STEP, SEQ_STEP)
        return (pltpu.make_async_copy(k_hbm.at[part], kbuf.at[slot], ki_sem.at[slot]),
                pltpu.make_async_copy(v_hbm.at[part], vbuf.at[slot], vi_sem.at[slot]))

    def out_copies(i):
        slot = lax.rem(i, SEQ_SLOTS)
        part = pl.ds(i * SEQ_STEP, SEQ_STEP)
        return (pltpu.make_async_copy(kbuf.at[slot], ko_hbm.at[part], ko_sem.at[slot]),
                pltpu.make_async_copy(vbuf.at[slot], vo_hbm.at[part], vo_sem.at[slot]))

    for i in range(QKV_SLOTS):
        w_copy(i).start()
    n_scr[...] = rms_norm(x_ref[...].astype(F32), gain_ref[...])
    q_scr[:, pl.ds(q_heads, HEAD_ROWS - q_heads), :] = jnp.zeros((rows, HEAD_ROWS - q_heads, HEAD), F32)
    even = lax.rem(lax.broadcasted_iota(jnp.int32, (rows, HEAD), 1), 2) == 0
    cosine = cos_ref[...]
    sine = sin_ref[...]

    for i in range(blocks):
        w_copy(i).wait()
        part = jnp.dot(n_scr[...], wbuf[i % QKV_SLOTS], preferred_element_type=F32)
        part = part + bias_ref[:, pl.ds(i * QKV_COLS, QKV_COLS)].astype(F32)
        if i + QKV_SLOTS < blocks:
            w_copy(i + QKV_SLOTS).start()
        elif i + QKV_SLOTS - blocks < 2:
            for copy in in_copies(i + QKV_SLOTS - blocks):
                copy.start()
        for j in range(heads_per_block):
            head = i * heads_per_block + j
            vals = part[:, j * HEAD:(j + 1) * HEAD]
            if head < q_heads + kv_heads:
                other = jnp.where(even, pltpu.roll(vals, HEAD - 1, 1), pltpu.roll(vals, 1, 1))
                vals = vals * cosine + other * sine
            if head < q_heads:
                q_scr[:, head, :] = vals
            elif head < q_heads + kv_heads:
                for rep in range(8 // kv_heads):
                    kn_scr[:, rep * kv_heads + head - q_heads, :] = vals
            else:
                for rep in range(8 // kv_heads):
                    vn_scr[:, rep * kv_heads + head - q_heads - kv_heads, :] = vals

    cols = kbuf.shape[2]
    col = lax.broadcasted_iota(jnp.int32, (HEAD_ROWS, cols), 1)
    row_group = jnp.minimum(lax.broadcasted_iota(jnp.int32, (HEAD_ROWS, cols), 0) // group, kv_heads - 1)
    own_group = lax.rem(col, kv_heads) == row_group
    positions = 16 // kv_heads

    def attend(i, carry):
        slot = lax.rem(i, SEQ_SLOTS)

        @pl.when(i >= 2)
        def _():
            for copy in out_copies(i - 2):
                copy.wait()

        @pl.when(i + 2 < steps)
        def _():
            for copy in in_copies(i + 2):
                copy.start()

        for copy in in_copies(i):
            copy.wait()
        lengths = [len_ref[i * SEQ_STEP + s] for s in range(SEQ_STEP)]
        new_row = lax.broadcasted_iota(jnp.int32, (16, HEAD), 0) // kv_heads
        for s in range(SEQ_STEP):
            base = pl.multiple_of((lengths[s] // positions) * 16, 16)
            hit = new_row == lax.rem(lengths[s], positions)
            for buf, new in ((kbuf, kn_scr), (vbuf, vn_scr)):
                fresh = new[i * SEQ_STEP + s]
                fresh = jnp.concatenate([fresh, fresh], axis=0).astype(BF16).astype(F32)
                old = buf[slot, s, pl.ds(base, 16), :].astype(F32)
                buf[slot, s, pl.ds(base, 16), :] = jnp.where(hit, fresh, old).astype(BF16)
        scores = [lax.dot_general(q_scr[i * SEQ_STEP + s].astype(BF16), kbuf[slot, s], (((1,), (1,)), ((), ())),
                                  preferred_element_type=F32) for s in range(SEQ_STEP)]
        for s in range(SEQ_STEP):
            seen = jnp.logical_and(own_group, col < (lengths[s] + 1) * kv_heads)
            logits = jnp.where(seen, scores[s] * (HEAD ** -0.5 * LOG2E), -jnp.inf)
            top = jnp.max(logits, axis=-1, keepdims=True)
            weights = jnp.exp2(logits - top)
            total = jnp.sum(weights, axis=-1, keepdims=True)
            probs = (weights * (1.0 / total)).astype(BF16)
            ctx_ref[i * SEQ_STEP + s] = jnp.dot(probs, vbuf[slot, s], preferred_element_type=F32)
        for copy in out_copies(i):
            copy.start()
        return carry

    lax.fori_loop(0, steps, attend, 0)
    for i in (steps - 2, steps - 1):
        for copy in out_copies(i):
            copy.wait()


def mlp_kernel(q_heads, ctx_ref, x_ref, gain_ref, wp_hbm, wi_hbm, wo_hbm, y_ref,
               ring, oring, m_all, ctx2, hid, act, send_d, recv_d, keep, send_i, recv_i,
               ring_sem, oring_sem, agx_s, agx_r, agp_s, agp_r, fwd_s, fwd_r, rsd_s, rsd_r, rsi_s, rsi_r):
    rows, width = x_ref.shape
    ffn = wo_hbm.shape[0]
    me = lax.axis_index("grp")
    partner = {"grp": me + 1 - 2 * lax.rem(me, 2)}
    cross = {"grp": lax.rem(me + 2, 4)}
    proj_blocks = wp_hbm.shape[0] // 2
    full = ffn // FF_BLOCK
    rest = ffn - full * FF_BLOCK
    chunks = width // OUT_COLS

    barrier = pltpu.get_barrier_semaphore()
    for peer in (partner, cross):
        pl.semaphore_signal(barrier, inc=1, device_id=peer, device_id_type=MESH)

    def proj_copy(i):
        return pltpu.make_async_copy(wp_hbm.at[pl.ds(2 * i, 2)], ring.at[i], ring_sem.at[i])

    def in_copy(j):
        slot = lax.rem(j, FF_SLOTS)
        return pltpu.make_async_copy(wi_hbm.at[:, pl.ds(pl.multiple_of(j * FF_BLOCK, FF_BLOCK), FF_BLOCK), :],
                                     ring.at[slot], ring_sem.at[slot])

    def rest_copy():
        slot = full % FF_SLOTS
        return pltpu.make_async_copy(wi_hbm.at[:, pl.ds(full * FF_BLOCK, rest), :],
                                     ring.at[slot, :, pl.ds(0, rest), :], ring_sem.at[slot])

    def out_copy(c):
        slot = lax.rem(c, OUT_SLOTS)
        return pltpu.make_async_copy(wo_hbm.at[:, pl.ds(pl.multiple_of(c * OUT_COLS, OUT_COLS), OUT_COLS)],
                                     oring.at[slot], oring_sem.at[slot])

    for i in range(proj_blocks):
        proj_copy(i).start()
    for head in range(q_heads):
        ctx2[:, pl.ds(head * HEAD, HEAD)] = ctx_ref[:, head, :].astype(BF16)
    hid[...] = x_ref[...].astype(F32)

    def project(i, carry):
        proj_copy(i).wait()
        block = ring[i].reshape(2 * FF_BLOCK, width)
        left = ctx2[:, pl.ds(pl.multiple_of(i * 2 * FF_BLOCK, 2 * FF_BLOCK), 2 * FF_BLOCK)]
        hid[...] += jnp.dot(left, block, preferred_element_type=F32)
        in_copy(i).start()
        return carry

    lax.fori_loop(0, proj_blocks, project, 0)
    out_copy(0).start()
    out_copy(1).start()
    m_all[pl.ds(0, rows), :] = rms_norm(hid[...], gain_ref[...])
    pl.semaphore_wait(barrier, 2)

    piece = rows // AG_CHUNKS

    def remote(src, dst, send, recv, peer):
        return pltpu.make_async_remote_copy(src_ref=src, dst_ref=dst, send_sem=send, recv_sem=recv,
                                            device_id=peer, device_id_type=MESH)

    to_cross = [remote(m_all.at[pl.ds(k * piece, piece)], m_all.at[pl.ds(rows + k * piece, piece)],
                       agx_s.at[k], agx_r.at[k], cross) for k in range(AG_CHUNKS)]
    to_partner = remote(m_all.at[pl.ds(0, rows)], m_all.at[pl.ds(2 * rows, rows)], agp_s, agp_r, partner)
    forward = [remote(m_all.at[pl.ds(rows + k * piece, piece)], m_all.at[pl.ds(3 * rows + k * piece, piece)],
                      fwd_s.at[k], fwd_r.at[k], partner) for k in range(AG_CHUNKS)]
    for copy in to_cross:
        copy.start()
    to_partner.start()
    for k in range(AG_CHUNKS):
        to_cross[k].wait_recv()
        forward[k].start()
    to_partner.wait_recv()
    for k in range(AG_CHUNKS):
        forward[k].wait_recv()

    def swiglu(gate, up):
        return (gate / (1.0 + jnp.exp(-gate)) * up).astype(BF16)

    contract_last = (((1,), (1,)), ((), ()))

    def gate_up(j, carry):
        slot = lax.rem(j, FF_SLOTS)
        in_copy(j).wait()
        gate = lax.dot_general(m_all[...], ring[slot, 0], contract_last, preferred_element_type=F32)
        up = lax.dot_general(m_all[...], ring[slot, 1], contract_last, preferred_element_type=F32)
        act[:, pl.ds(pl.multiple_of(j * FF_BLOCK, FF_BLOCK), FF_BLOCK)] = swiglu(gate, up)

        @pl.when(j + FF_SLOTS < full)
        def _():
            in_copy(j + FF_SLOTS).start()

        @pl.when(j + FF_SLOTS == full)
        def _():
            rest_copy().start()

        for c in range(2, OUT_SLOTS):
            @pl.when(j == 3 * (c - 1))
            def _():
                out_copy(c).start()

        return carry

    lax.fori_loop(0, full, gate_up, 0)
    rest_copy().wait()
    slot = full % FF_SLOTS
    gate = lax.dot_general(m_all[...], ring[slot, 0, pl.ds(0, rest), :], contract_last, preferred_element_type=F32)
    up = lax.dot_general(m_all[...], ring[slot, 1, pl.ds(0, rest), :], contract_last, preferred_element_type=F32)
    act[:, pl.ds(full * FF_BLOCK, rest)] = swiglu(gate, up)

    def die_copy(c):
        return remote(send_d.at[c], recv_d.at[c], rsd_s.at[c], rsd_r.at[c], partner)

    def chip_copy(c):
        return remote(send_i.at[c], recv_i.at[c], rsi_s.at[c], rsi_r.at[c], cross)

    def finish(c):
        cols = pl.ds(pl.multiple_of(c * OUT_COLS, OUT_COLS), OUT_COLS)
        die_copy(c).wait_recv()
        chip_sum = keep[lax.rem(c, 2)] + recv_d[c].astype(F32)
        send_i[c] = chip_sum[rows:].astype(BF16)
        hid[:, cols] += chip_sum[:rows]
        chip_copy(c).start()

    def down(c, carry):
        out_copy(c).wait()
        part = jnp.dot(act[...], oring[lax.rem(c, OUT_SLOTS)], preferred_element_type=F32)

        @pl.when(c + OUT_SLOTS < chunks)
        def _():
            out_copy(c + OUT_SLOTS).start()

        send_d[c] = part[2 * rows:].astype(BF16)
        keep[lax.rem(c, 2)] = part[:2 * rows]
        die_copy(c).start()

        @pl.when(c > 0)
        def _():
            finish(c - 1)

        return carry

    lax.fori_loop(0, chunks, down, 0)
    finish(chunks - 1)
    for c in range(chunks):
        cols = pl.ds(c * OUT_COLS, OUT_COLS)
        chip_copy(c).wait_recv()
        y_ref[:, cols] = (hid[:, cols] + recv_i[c].astype(F32)).astype(BF16)
    for copy in (*to_cross, to_partner, *forward):
        copy.wait_send()
    for c in range(chunks):
        die_copy(c).wait_send()
        chip_copy(c).wait_send()


def solution(mesh):
    row_spec = P(('rep', 'grp'))
    repl_spec = P()
    vmem = pl.BlockSpec(memory_space=pltpu.VMEM)
    smem = pl.BlockSpec(memory_space=pltpu.SMEM)
    hbm = pl.BlockSpec(memory_space=pl.ANY)
    dma = pltpu.SemaphoreType.DMA

    def local_layer(x_in, seq_len, k_cache, v_cache, gamma_attn, w_qkv, b_qkv, w_proj, gamma_mlp, w_in, w_out):
        rows, width = x_in.shape
        cache_len, kv_heads = k_cache.shape[1:3]
        q_heads = w_proj.shape[0] // HEAD
        ffn = w_out.shape[0]
        cache_rows = cache_len * kv_heads

        rot_dim = HEAD // 2
        inv_freq = ROPE_BASE ** (-jnp.arange(0, rot_dim, 2, dtype=F32) / rot_dim)
        angles = seq_len.astype(F32)[:, None] * jnp.repeat(inv_freq, 2)[None, :]
        sign = jnp.where(jnp.arange(rot_dim) % 2 == 0, -1.0, 1.0).astype(F32)
        cosine = jnp.concatenate([jnp.cos(angles), jnp.ones((rows, HEAD - rot_dim), F32)], axis=1)
        sine = jnp.concatenate([jnp.sin(angles) * sign, jnp.zeros((rows, HEAD - rot_dim), F32)], axis=1)

        flat = jax.ShapeDtypeStruct((rows, cache_rows, HEAD), BF16)
        context, k_out, v_out = pl.pallas_call(
            functools.partial(qkv_attention_kernel, q_heads, kv_heads),
            out_shape=(jax.ShapeDtypeStruct((rows, HEAD_ROWS, HEAD), F32), flat, flat),
            in_specs=[smem, vmem, vmem, vmem, vmem, vmem, hbm, hbm, hbm],
            out_specs=(vmem, hbm, hbm),
            scratch_shapes=[
                pltpu.VMEM((QKV_SLOTS, width, QKV_COLS), BF16),
                pltpu.VMEM((SEQ_SLOTS, SEQ_STEP, cache_rows, HEAD), BF16),
                pltpu.VMEM((SEQ_SLOTS, SEQ_STEP, cache_rows, HEAD), BF16),
                pltpu.VMEM((rows, width), BF16),
                pltpu.VMEM((rows, HEAD_ROWS, HEAD), F32),
                pltpu.VMEM((rows, 8, HEAD), F32),
                pltpu.VMEM((rows, 8, HEAD), F32),
                dma((QKV_SLOTS,)), dma((SEQ_SLOTS,)), dma((SEQ_SLOTS,)), dma((SEQ_SLOTS,)), dma((SEQ_SLOTS,)),
            ],
            compiler_params=pltpu.CompilerParams(vmem_limit_bytes=60 * 1024 * 1024),
            name="qkv_attention",
        )(seq_len, x_in, gamma_attn.reshape(1, width), b_qkv.reshape(1, -1), cosine, sine, w_qkv,
          k_cache.reshape(rows, cache_rows, HEAD), v_cache.reshape(rows, cache_rows, HEAD))

        chunks = width // OUT_COLS
        layer_out = pl.pallas_call(
            functools.partial(mlp_kernel, q_heads),
            out_shape=jax.ShapeDtypeStruct((rows, width), BF16),
            in_specs=[vmem, vmem, vmem, hbm, hbm, hbm],
            out_specs=vmem,
            scratch_shapes=[
                pltpu.VMEM((FF_SLOTS, 2, FF_BLOCK, width), BF16),
                pltpu.VMEM((OUT_SLOTS, ffn, OUT_COLS), BF16),
                pltpu.VMEM((4 * rows, width), BF16),
                pltpu.VMEM((rows, width), BF16),
                pltpu.VMEM((rows, width), F32),
                pltpu.VMEM((4 * rows, ffn), BF16),
                pltpu.VMEM((chunks, 2 * rows, OUT_COLS), BF16),
                pltpu.VMEM((chunks, 2 * rows, OUT_COLS), BF16),
                pltpu.VMEM((2, 2 * rows, OUT_COLS), F32),
                pltpu.VMEM((chunks, rows, OUT_COLS), BF16),
                pltpu.VMEM((chunks, rows, OUT_COLS), BF16),
                dma((FF_SLOTS,)), dma((OUT_SLOTS,)),
                dma((AG_CHUNKS,)), dma((AG_CHUNKS,)), dma, dma, dma((AG_CHUNKS,)), dma((AG_CHUNKS,)),
                dma((chunks,)), dma((chunks,)), dma((chunks,)), dma((chunks,)),
            ],
            compiler_params=pltpu.CompilerParams(collective_id=0, has_side_effects=True,
                                                 vmem_limit_bytes=67043328),
            name="proj_mlp",
        )(context, x_in, gamma_mlp.reshape(1, width), w_proj.reshape(-1, FF_BLOCK, width), w_in, w_out)
        return layer_out, k_out.reshape(k_cache.shape), v_out.reshape(v_cache.shape)

    return jax.shard_map(local_layer, mesh=mesh,
                         in_specs=(row_spec, row_spec, row_spec, row_spec, repl_spec, repl_spec, repl_spec,
                                   repl_spec, repl_spec, P(None, 'grp', None), P('grp', None)),
                         out_specs=(row_spec, row_spec, row_spec), check_vma=False)
```

```python
import functools
import math

import jax
import jax.numpy as jnp
from jax import lax
from jax.experimental import pallas as pl
from jax.experimental.pallas import tpu as pltpu
from jax.sharding import PartitionSpec as P

HEAD = 128
ROPE_BASE = 10000.0
EPS = 1e-5
MESH = pl.DeviceIdType.MESH
F32 = jnp.float32
BF16 = jnp.bfloat16
LOG2E = 1.4426950408889634

QKV_COLS = 512
QKV_SLOTS = 4
SEQ_STEP = 4
SEQ_SLOTS = 4
HEAD_ROWS = 32
FF_BLOCK = 256
FF_SLOTS = 7
FF_UNROLL = 3
OUT_COLS = 512
OUT_SLOTS = 5
AG_CHUNKS = 4


def rms_norm(vals, gain):
    mean_sq = jnp.mean(vals * vals, axis=-1, keepdims=True)
    return (vals * lax.rsqrt(mean_sq + EPS) * gain.astype(F32).reshape(1, -1)).astype(BF16)


def rotary_tables(len_ref, table, rows):
    rot_dim = HEAD // 2
    for b in range(rows):
        table[pl.ds(b, 1), :] = jnp.full((1, HEAD), len_ref[b], jnp.int32).astype(F32)
    dim = lax.broadcasted_iota(jnp.int32, (1, HEAD), 1)
    pair = (dim // 2 * 2).astype(F32)
    inv_freq = jnp.where(dim < rot_dim, jnp.exp(pair * (-math.log(ROPE_BASE) / rot_dim)), 0.0)
    angles = table[...] * inv_freq
    sine = jnp.sin(angles)
    return jnp.cos(angles), jnp.where(lax.rem(dim, 2) == 0, -sine, sine)


def qkv_attention_kernel(q_heads, kv_heads, len_ref, x_ref, gain_ref, bias_ref, w_hbm, k_hbm, v_hbm,
                         ctx_ref, ko_hbm, vo_hbm, wbuf, kbuf, vbuf, table, n_scr, q_scr, kn_scr, vn_scr,
                         w_sem, ki_sem, vi_sem, ko_sem, vo_sem):
    rows = x_ref.shape[0]
    blocks = w_hbm.shape[1] // QKV_COLS
    steps = rows // SEQ_STEP
    group = q_heads // kv_heads
    heads_per_block = QKV_COLS // HEAD

    def w_copy(i):
        return pltpu.make_async_copy(w_hbm.at[:, pl.ds(i * QKV_COLS, QKV_COLS)], wbuf.at[i % QKV_SLOTS],
                                     w_sem.at[i % QKV_SLOTS])

    def in_copies(i):
        slot = lax.rem(i, SEQ_SLOTS)
        part = pl.ds(i * SEQ_STEP, SEQ_STEP)
        return (pltpu.make_async_copy(k_hbm.at[part], kbuf.at[slot], ki_sem.at[slot]),
                pltpu.make_async_copy(v_hbm.at[part], vbuf.at[slot], vi_sem.at[slot]))

    def out_copies(i):
        slot = lax.rem(i, SEQ_SLOTS)
        part = pl.ds(i * SEQ_STEP, SEQ_STEP)
        return (pltpu.make_async_copy(kbuf.at[slot], ko_hbm.at[part], ko_sem.at[slot]),
                pltpu.make_async_copy(vbuf.at[slot], vo_hbm.at[part], vo_sem.at[slot]))

    for i in range(QKV_SLOTS):
        w_copy(i).start()
    n_scr[...] = rms_norm(x_ref[...].astype(F32), gain_ref[...])
    q_scr[:, pl.ds(q_heads, HEAD_ROWS - q_heads), :] = jnp.zeros((rows, HEAD_ROWS - q_heads, HEAD), F32)
    even = lax.rem(lax.broadcasted_iota(jnp.int32, (rows, HEAD), 1), 2) == 0
    cosine, sine = rotary_tables(len_ref, table, rows)

    for i in range(blocks):
        w_copy(i).wait()
        part = jnp.dot(n_scr[...], wbuf[i % QKV_SLOTS], preferred_element_type=F32)
        part = part + bias_ref[pl.ds(i * QKV_COLS, QKV_COLS)].astype(F32).reshape(1, -1)
        if i + QKV_SLOTS < blocks:
            w_copy(i + QKV_SLOTS).start()
        elif i + QKV_SLOTS - blocks < 2:
            for copy in in_copies(i + QKV_SLOTS - blocks):
                copy.start()
        for j in range(heads_per_block):
            head = i * heads_per_block + j
            vals = part[:, j * HEAD:(j + 1) * HEAD]
            if head < q_heads + kv_heads:
                other = jnp.where(even, pltpu.roll(vals, HEAD - 1, 1), pltpu.roll(vals, 1, 1))
                vals = vals * cosine + other * sine
            if head < q_heads:
                q_scr[:, head, :] = vals
            elif head < q_heads + kv_heads:
                for rep in range(8 // kv_heads):
                    kn_scr[:, rep * kv_heads + head - q_heads, :] = vals
            else:
                for rep in range(8 // kv_heads):
                    vn_scr[:, rep * kv_heads + head - q_heads - kv_heads, :] = vals

    cols = kbuf.shape[2]
    col = lax.broadcasted_iota(jnp.int32, (HEAD_ROWS, cols), 1)
    row_group = jnp.minimum(lax.broadcasted_iota(jnp.int32, (HEAD_ROWS, cols), 0) // group, kv_heads - 1)
    own_group = lax.rem(col, kv_heads) == row_group
    positions = 16 // kv_heads

    def attend(i, carry):
        slot = lax.rem(i, SEQ_SLOTS)

        @pl.when(i >= 2)
        def _():
            for copy in out_copies(i - 2):
                copy.wait()

        @pl.when(i + 2 < steps)
        def _():
            for copy in in_copies(i + 2):
                copy.start()

        for copy in in_copies(i):
            copy.wait()
        lengths = [len_ref[i * SEQ_STEP + s] for s in range(SEQ_STEP)]
        new_row = lax.broadcasted_iota(jnp.int32, (16, HEAD), 0) // kv_heads
        for s in range(SEQ_STEP):
            base = pl.multiple_of((lengths[s] // positions) * 16, 16)
            hit = new_row == lax.rem(lengths[s], positions)
            for buf, new in ((kbuf, kn_scr), (vbuf, vn_scr)):
                fresh = new[i * SEQ_STEP + s]
                fresh = jnp.concatenate([fresh, fresh], axis=0).astype(BF16).astype(F32)
                old = buf[slot, s, pl.ds(base, 16), :].astype(F32)
                buf[slot, s, pl.ds(base, 16), :] = jnp.where(hit, fresh, old).astype(BF16)
        scores = [lax.dot_general(q_scr[i * SEQ_STEP + s].astype(BF16), kbuf[slot, s], (((1,), (1,)), ((), ())),
                                  preferred_element_type=F32) for s in range(SEQ_STEP)]
        for s in range(SEQ_STEP):
            seen = jnp.logical_and(own_group, col < (lengths[s] + 1) * kv_heads)
            logits = jnp.where(seen, scores[s] * (HEAD ** -0.5 * LOG2E), -jnp.inf)
            top = jnp.max(logits, axis=-1, keepdims=True)
            weights = jnp.exp2(logits - top)
            total = jnp.sum(weights, axis=-1, keepdims=True)
            probs = (weights * (1.0 / total)).astype(BF16)
            ctx_ref[i * SEQ_STEP + s] = jnp.dot(probs, vbuf[slot, s], preferred_element_type=F32)
        for copy in out_copies(i):
            copy.start()
        return carry

    lax.fori_loop(0, steps, attend, 0)
    for i in (steps - 2, steps - 1):
        for copy in out_copies(i):
            copy.wait()


def mlp_kernel(q_heads, ctx_ref, x_ref, gain_ref, wp_hbm, wi_hbm, wo_hbm, y_ref,
               ring, oring, m_all, ctx2, hid, act, send_d, recv_d, keep, send_i, recv_i,
               ring_sem, oring_sem, agx_s, agx_r, agp_s, agp_r, fwd_s, fwd_r, rsd_s, rsd_r, rsi_s, rsi_r):
    rows, width = x_ref.shape
    ffn = wo_hbm.shape[0]
    me = lax.axis_index("grp")
    partner = {"grp": me + 1 - 2 * lax.rem(me, 2)}
    cross = {"grp": lax.rem(me + 2, 4)}
    proj_blocks = wp_hbm.shape[0] // 2
    full = ffn // FF_BLOCK
    rest = ffn - full * FF_BLOCK
    chunks = width // OUT_COLS

    barrier = pltpu.get_barrier_semaphore()
    for peer in (partner, cross):
        pl.semaphore_signal(barrier, inc=1, device_id=peer, device_id_type=MESH)

    def proj_copy(i):
        return pltpu.make_async_copy(wp_hbm.at[pl.ds(2 * i, 2)], ring.at[i], ring_sem.at[i])

    def in_copy(j):
        slot = lax.rem(j, FF_SLOTS)
        return pltpu.make_async_copy(wi_hbm.at[:, pl.ds(pl.multiple_of(j * FF_BLOCK, FF_BLOCK), FF_BLOCK), :],
                                     ring.at[slot], ring_sem.at[slot])

    def rest_copy():
        slot = full % FF_SLOTS
        return pltpu.make_async_copy(wi_hbm.at[:, pl.ds(full * FF_BLOCK, rest), :],
                                     ring.at[slot, :, pl.ds(0, rest), :], ring_sem.at[slot])

    def out_copy(c):
        slot = lax.rem(c, OUT_SLOTS)
        return pltpu.make_async_copy(wo_hbm.at[:, pl.ds(pl.multiple_of(c * OUT_COLS, OUT_COLS), OUT_COLS)],
                                     oring.at[slot], oring_sem.at[slot])

    for i in range(proj_blocks):
        proj_copy(i).start()
    for head in range(q_heads):
        ctx2[:, pl.ds(head * HEAD, HEAD)] = ctx_ref[:, head, :].astype(BF16)
    hid[...] = x_ref[...].astype(F32)

    def project(i, carry):
        proj_copy(i).wait()
        block = ring[i].reshape(2 * FF_BLOCK, width)
        left = ctx2[:, pl.ds(pl.multiple_of(i * 2 * FF_BLOCK, 2 * FF_BLOCK), 2 * FF_BLOCK)]
        hid[...] += jnp.dot(left, block, preferred_element_type=F32)
        in_copy(i).start()
        return carry

    lax.fori_loop(0, proj_blocks, project, 0)
    out_copy(0).start()
    out_copy(1).start()
    m_all[pl.ds(0, rows), :] = rms_norm(hid[...], gain_ref[...])
    pl.semaphore_wait(barrier, 2)

    piece = rows // AG_CHUNKS

    def remote(src, dst, send, recv, peer):
        return pltpu.make_async_remote_copy(src_ref=src, dst_ref=dst, send_sem=send, recv_sem=recv,
                                            device_id=peer, device_id_type=MESH)

    to_cross = [remote(m_all.at[pl.ds(k * piece, piece)], m_all.at[pl.ds(rows + k * piece, piece)],
                       agx_s.at[k], agx_r.at[k], cross) for k in range(AG_CHUNKS)]
    to_partner = remote(m_all.at[pl.ds(0, rows)], m_all.at[pl.ds(2 * rows, rows)], agp_s, agp_r, partner)
    forward = [remote(m_all.at[pl.ds(rows + k * piece, piece)], m_all.at[pl.ds(3 * rows + k * piece, piece)],
                      fwd_s.at[k], fwd_r.at[k], partner) for k in range(AG_CHUNKS)]
    for copy in to_cross:
        copy.start()
    to_partner.start()
    for k in range(AG_CHUNKS):
        to_cross[k].wait_recv()
        forward[k].start()
    to_partner.wait_recv()
    for k in range(AG_CHUNKS):
        forward[k].wait_recv()

    def swiglu(gate, up):
        return (gate / (1.0 + jnp.exp(-gate)) * up).astype(BF16)

    contract_last = (((1,), (1,)), ((), ()))

    def gate_up(t, carry):
        for k in range(FF_UNROLL):
            in_copy(t * FF_UNROLL + k).wait()
        for k in range(FF_UNROLL):
            j = t * FF_UNROLL + k
            slot = lax.rem(j, FF_SLOTS)
            gate = lax.dot_general(m_all[...], ring[slot, 0], contract_last, preferred_element_type=F32)
            up = lax.dot_general(m_all[...], ring[slot, 1], contract_last, preferred_element_type=F32)
            act[:, pl.ds(pl.multiple_of(j * FF_BLOCK, FF_BLOCK), FF_BLOCK)] = swiglu(gate, up)
        for k in range(FF_UNROLL):
            j = t * FF_UNROLL + k

            @pl.when(j + FF_SLOTS < full)
            def _():
                in_copy(j + FF_SLOTS).start()

            @pl.when(j + FF_SLOTS == full)
            def _():
                rest_copy().start()

        for c in range(2, OUT_SLOTS):
            @pl.when(t == c - 1)
            def _():
                out_copy(c).start()

        return carry

    lax.fori_loop(0, full // FF_UNROLL, gate_up, 0)
    rest_copy().wait()
    slot = full % FF_SLOTS
    gate = lax.dot_general(m_all[...], ring[slot, 0, pl.ds(0, rest), :], contract_last, preferred_element_type=F32)
    up = lax.dot_general(m_all[...], ring[slot, 1, pl.ds(0, rest), :], contract_last, preferred_element_type=F32)
    act[:, pl.ds(full * FF_BLOCK, rest)] = swiglu(gate, up)

    def die_copy(c):
        return remote(send_d.at[c], recv_d.at[c], rsd_s.at[c], rsd_r.at[c], partner)

    def chip_copy(c):
        return remote(send_i.at[c], recv_i.at[c], rsi_s.at[c], rsi_r.at[c], cross)

    def finish(c):
        cols = pl.ds(pl.multiple_of(c * OUT_COLS, OUT_COLS), OUT_COLS)
        die_copy(c).wait_recv()
        chip_sum = keep[lax.rem(c, 2)] + recv_d[c].astype(F32)
        send_i[c] = chip_sum[rows:].astype(BF16)
        hid[:, cols] += chip_sum[:rows]
        chip_copy(c).start()

    def down(c, carry):
        out_copy(c).wait()
        part = jnp.dot(act[...], oring[lax.rem(c, OUT_SLOTS)], preferred_element_type=F32)

        @pl.when(c + OUT_SLOTS < chunks)
        def _():
            out_copy(c + OUT_SLOTS).start()

        send_d[c] = part[2 * rows:].astype(BF16)
        keep[lax.rem(c, 2)] = part[:2 * rows]
        die_copy(c).start()

        @pl.when(c > 0)
        def _():
            finish(c - 1)

        return carry

    lax.fori_loop(0, chunks, down, 0)
    finish(chunks - 1)
    for c in range(chunks):
        cols = pl.ds(c * OUT_COLS, OUT_COLS)
        chip_copy(c).wait_recv()
        y_ref[:, cols] = (hid[:, cols] + recv_i[c].astype(F32)).astype(BF16)
    for copy in (*to_cross, to_partner, *forward):
        copy.wait_send()
    for c in range(chunks):
        die_copy(c).wait_send()
        chip_copy(c).wait_send()


def solution(mesh):
    row_spec = P(('rep', 'grp'))
    repl_spec = P()
    vmem = pl.BlockSpec(memory_space=pltpu.VMEM)
    smem = pl.BlockSpec(memory_space=pltpu.SMEM)
    hbm = pl.BlockSpec(memory_space=pl.ANY)
    dma = pltpu.SemaphoreType.DMA

    def local_layer(x_in, seq_len, k_cache, v_cache, gamma_attn, w_qkv, b_qkv, w_proj, gamma_mlp, w_in, w_out):
        rows, width = x_in.shape
        cache_len, kv_heads = k_cache.shape[1:3]
        q_heads = w_proj.shape[0] // HEAD
        ffn = w_out.shape[0]
        cache_rows = cache_len * kv_heads

        flat = jax.ShapeDtypeStruct((rows, cache_rows, HEAD), BF16)
        context, k_out, v_out = pl.pallas_call(
            functools.partial(qkv_attention_kernel, q_heads, kv_heads),
            out_shape=(jax.ShapeDtypeStruct((rows, HEAD_ROWS, HEAD), F32), flat, flat),
            in_specs=[smem, vmem, vmem, vmem, hbm, hbm, hbm],
            out_specs=(vmem, hbm, hbm),
            scratch_shapes=[
                pltpu.VMEM((QKV_SLOTS, width, QKV_COLS), BF16),
                pltpu.VMEM((SEQ_SLOTS, SEQ_STEP, cache_rows, HEAD), BF16),
                pltpu.VMEM((SEQ_SLOTS, SEQ_STEP, cache_rows, HEAD), BF16),
                pltpu.VMEM((rows, HEAD), F32),
                pltpu.VMEM((rows, width), BF16),
                pltpu.VMEM((rows, HEAD_ROWS, HEAD), F32),
                pltpu.VMEM((rows, 8, HEAD), F32),
                pltpu.VMEM((rows, 8, HEAD), F32),
                dma((QKV_SLOTS,)), dma((SEQ_SLOTS,)), dma((SEQ_SLOTS,)), dma((SEQ_SLOTS,)), dma((SEQ_SLOTS,)),
            ],
            compiler_params=pltpu.CompilerParams(vmem_limit_bytes=60 * 1024 * 1024),
            name="qkv_attention",
        )(seq_len, x_in, gamma_attn, b_qkv, w_qkv,
          k_cache.reshape(rows, cache_rows, HEAD), v_cache.reshape(rows, cache_rows, HEAD))

        chunks = width // OUT_COLS
        layer_out = pl.pallas_call(
            functools.partial(mlp_kernel, q_heads),
            out_shape=jax.ShapeDtypeStruct((rows, width), BF16),
            in_specs=[vmem, vmem, vmem, hbm, hbm, hbm],
            out_specs=vmem,
            scratch_shapes=[
                pltpu.VMEM((FF_SLOTS, 2, FF_BLOCK, width), BF16),
                pltpu.VMEM((OUT_SLOTS, ffn, OUT_COLS), BF16),
                pltpu.VMEM((4 * rows, width), BF16),
                pltpu.VMEM((rows, width), BF16),
                pltpu.VMEM((rows, width), F32),
                pltpu.VMEM((4 * rows, ffn), BF16),
                pltpu.VMEM((chunks, 2 * rows, OUT_COLS), BF16),
                pltpu.VMEM((chunks, 2 * rows, OUT_COLS), BF16),
                pltpu.VMEM((2, 2 * rows, OUT_COLS), F32),
                pltpu.VMEM((chunks, rows, OUT_COLS), BF16),
                pltpu.VMEM((chunks, rows, OUT_COLS), BF16),
                dma((FF_SLOTS,)), dma((OUT_SLOTS,)),
                dma((AG_CHUNKS,)), dma((AG_CHUNKS,)), dma, dma, dma((AG_CHUNKS,)), dma((AG_CHUNKS,)),
                dma((chunks,)), dma((chunks,)), dma((chunks,)), dma((chunks,)),
            ],
            compiler_params=pltpu.CompilerParams(collective_id=0, has_side_effects=True,
                                                 vmem_limit_bytes=67043328),
            name="proj_mlp",
        )(context, x_in, gamma_mlp, w_proj.reshape(-1, FF_BLOCK, width), w_in, w_out)
        return layer_out, k_out.reshape(k_cache.shape), v_out.reshape(v_cache.shape)

    return jax.shard_map(local_layer, mesh=mesh,
                         in_specs=(row_spec, row_spec, row_spec, row_spec, repl_spec, repl_spec, repl_spec,
                                   repl_spec, repl_spec, P(None, 'grp', None), P('grp', None)),
                         out_specs=(row_spec, row_spec, row_spec), check_vma=False)
```

```python
import functools
import math

import jax
import jax.numpy as jnp
from jax import lax
from jax.experimental import pallas as pl
from jax.experimental.pallas import tpu as pltpu
from jax.sharding import PartitionSpec as P

HEAD = 128
ROPE_BASE = 10000.0
EPS = 1e-5
MESH = pl.DeviceIdType.MESH
F32 = jnp.float32
BF16 = jnp.bfloat16
LOG2E = 1.4426950408889634

QKV_COLS = 512
QKV_SLOTS = 4
SEQ_STEP = 4
SEQ_SLOTS = 4
HEAD_ROWS = 32
FF_BLOCK = 256
FF_SLOTS = 8
FF_GROUPS = (2, 3, 3, 2)
OUT_COLS = 512
OUT_SLOTS = 5
AG_CHUNKS = 4


def rms_norm(vals, gain):
    mean_sq = jnp.mean(vals * vals, axis=-1, keepdims=True)
    return (vals * lax.rsqrt(mean_sq + EPS) * gain.astype(F32).reshape(1, -1)).astype(BF16)


def rotary_tables(len_ref, table, rows):
    rot_dim = HEAD // 2
    for b in range(rows):
        table[pl.ds(b, 1), :] = jnp.full((1, HEAD), len_ref[b], jnp.int32).astype(F32)
    dim = lax.broadcasted_iota(jnp.int32, (1, HEAD), 1)
    pair = (dim // 2 * 2).astype(F32)
    inv_freq = jnp.where(dim < rot_dim, jnp.exp(pair * (-math.log(ROPE_BASE) / rot_dim)), 0.0)
    angles = table[...] * inv_freq
    sine = jnp.sin(angles)
    return jnp.cos(angles), jnp.where(lax.rem(dim, 2) == 0, -sine, sine)


def attention_kernel(q_heads, kv_heads, len_hbm, x_hbm, gain_hbm, bias_hbm, gain2_hbm, w_hbm, wp_hbm, k_hbm, v_hbm,
                     m_ref, hid_ref, ko_hbm, vo_hbm,
                     len_ref, x_ref, gain_ref, bias_ref, gain2_ref, wbuf, kbuf, vbuf, table, n_scr, q_scr, kn_scr, vn_scr,
                     ctx_ref, small_sem, w_sem, ki_sem, vi_sem, ko_sem, vo_sem):
    rows, width = x_ref.shape
    blocks = w_hbm.shape[1] // QKV_COLS
    proj_blocks = wp_hbm.shape[1] // QKV_COLS
    steps = rows // SEQ_STEP
    group = q_heads // kv_heads
    heads_per_block = QKV_COLS // HEAD

    def proj_copy(i):
        return pltpu.make_async_copy(wp_hbm.at[:, pl.ds(i * QKV_COLS, QKV_COLS)], wbuf.at[i % QKV_SLOTS],
                                     w_sem.at[i % QKV_SLOTS])

    def w_copy(i):
        return pltpu.make_async_copy(w_hbm.at[:, pl.ds(i * QKV_COLS, QKV_COLS)], wbuf.at[i % QKV_SLOTS],
                                     w_sem.at[i % QKV_SLOTS])

    def in_copies(i):
        slot = lax.rem(i, SEQ_SLOTS)
        part = pl.ds(i * SEQ_STEP, SEQ_STEP)
        return (pltpu.make_async_copy(k_hbm.at[part], kbuf.at[slot], ki_sem.at[slot]),
                pltpu.make_async_copy(v_hbm.at[part], vbuf.at[slot], vi_sem.at[slot]))

    def out_copies(i):
        slot = lax.rem(i, SEQ_SLOTS)
        part = pl.ds(i * SEQ_STEP, SEQ_STEP)
        return (pltpu.make_async_copy(kbuf.at[slot], ko_hbm.at[part], ko_sem.at[slot]),
                pltpu.make_async_copy(vbuf.at[slot], vo_hbm.at[part], vo_sem.at[slot]))

    small = [pltpu.make_async_copy(src, dst, small_sem.at[i]) for i, (src, dst) in enumerate((
        (x_hbm, x_ref), (gain_hbm, gain_ref), (len_hbm, len_ref), (bias_hbm, bias_ref), (gain2_hbm, gain2_ref)))]
    for copy in small:
        copy.start()
    for i in range(QKV_SLOTS):
        w_copy(i).start(priority=1)
    q_scr[:, pl.ds(q_heads, HEAD_ROWS - q_heads), :] = jnp.zeros((rows, HEAD_ROWS - q_heads, HEAD), F32)
    for copy in small:
        copy.wait()
    n_scr[...] = rms_norm(x_ref[...].astype(F32), gain_ref[...])
    even = lax.rem(lax.broadcasted_iota(jnp.int32, (rows, HEAD), 1), 2) == 0
    cosine, sine = rotary_tables(len_ref, table, rows)

    for i in range(blocks):
        w_copy(i).wait()
        part = jnp.dot(n_scr[...], wbuf[i % QKV_SLOTS], preferred_element_type=F32)
        part = part + bias_ref[pl.ds(i * QKV_COLS, QKV_COLS)].astype(F32).reshape(1, -1)
        if i + QKV_SLOTS < blocks:
            w_copy(i + QKV_SLOTS).start(priority=1)
        elif i + QKV_SLOTS - blocks < 2:
            for copy in in_copies(i + QKV_SLOTS - blocks):
                copy.start()
        for j in range(heads_per_block):
            head = i * heads_per_block + j
            vals = part[:, j * HEAD:(j + 1) * HEAD]
            if head < q_heads + kv_heads:
                other = jnp.where(even, pltpu.roll(vals, HEAD - 1, 1), pltpu.roll(vals, 1, 1))
                vals = vals * cosine + other * sine
            if head < q_heads:
                q_scr[:, head, :] = vals
            elif head < q_heads + kv_heads:
                for rep in range(8 // kv_heads):
                    kn_scr[:, rep * kv_heads + head - q_heads, :] = vals
            else:
                for rep in range(8 // kv_heads):
                    vn_scr[:, rep * kv_heads + head - q_heads - kv_heads, :] = vals

    cols = kbuf.shape[2]
    col = lax.broadcasted_iota(jnp.int32, (HEAD_ROWS, cols), 1)
    row_group = jnp.minimum(lax.broadcasted_iota(jnp.int32, (HEAD_ROWS, cols), 0) // group, kv_heads - 1)
    own_group = lax.rem(col, kv_heads) == row_group
    positions = 16 // kv_heads

    def attend(i, carry):
        slot = lax.rem(i, SEQ_SLOTS)

        @pl.when(i >= 2)
        def _():
            for copy in out_copies(i - 2):
                copy.wait()

        @pl.when(i + 2 < steps)
        def _():
            for copy in in_copies(i + 2):
                copy.start()

        for copy in in_copies(i):
            copy.wait()
        lengths = [len_ref[i * SEQ_STEP + s] for s in range(SEQ_STEP)]
        new_row = lax.broadcasted_iota(jnp.int32, (16, HEAD), 0) // kv_heads
        for s in range(SEQ_STEP):
            base = pl.multiple_of((lengths[s] // positions) * 16, 16)
            hit = new_row == lax.rem(lengths[s], positions)
            for buf, new in ((kbuf, kn_scr), (vbuf, vn_scr)):
                fresh = new[i * SEQ_STEP + s]
                fresh = jnp.concatenate([fresh, fresh], axis=0).astype(BF16).astype(F32)
                old = buf[slot, s, pl.ds(base, 16), :].astype(F32)
                buf[slot, s, pl.ds(base, 16), :] = jnp.where(hit, fresh, old).astype(BF16)
        scores = [lax.dot_general(q_scr[i * SEQ_STEP + s].astype(BF16), kbuf[slot, s], (((1,), (1,)), ((), ())),
                                  preferred_element_type=F32) for s in range(SEQ_STEP)]
        for s in range(SEQ_STEP):
            seen = jnp.logical_and(own_group, col < (lengths[s] + 1) * kv_heads)
            logits = jnp.where(seen, scores[s] * (HEAD ** -0.5 * LOG2E), -jnp.inf)
            top = jnp.max(logits, axis=-1, keepdims=True)
            weights = jnp.exp2(logits - top)
            total = jnp.sum(weights, axis=-1, keepdims=True)
            probs = (weights * (1.0 / total)).astype(BF16)
            ctx_ref[i * SEQ_STEP + s] = jnp.dot(probs, vbuf[slot, s], preferred_element_type=F32)
        for copy in out_copies(i):
            copy.start()
        for n in range(QKV_SLOTS):
            @pl.when(i == steps - QKV_SLOTS + n)
            def _():
                proj_copy(n).start(priority=1)

        return carry

    lax.fori_loop(0, steps, attend, 0)
    for head in range(q_heads):
        n_scr[:, pl.ds(head * HEAD, HEAD)] = ctx_ref[:, head, :].astype(BF16)
    for i in range(proj_blocks):
        cols = pl.ds(i * QKV_COLS, QKV_COLS)
        proj_copy(i).wait()
        part = jnp.dot(n_scr[...], wbuf[i % QKV_SLOTS], preferred_element_type=F32)
        if i + QKV_SLOTS < proj_blocks:
            proj_copy(i + QKV_SLOTS).start(priority=1)
        hid_ref[:, cols] = x_ref[:, cols].astype(F32) + part
    m_ref[...] = rms_norm(hid_ref[...], gain2_ref[...])
    for i in (steps - 2, steps - 1):
        for copy in out_copies(i):
            copy.wait()


def mlp_kernel(m_hbm, hid_hbm, wi_hbm, wo_hbm, y_ref,
               ring, oring, m_all, hid, act, send_d, recv_d, keep, send_i, recv_i,
               m_sem, hid_sem, ring_sem, rest_sem, oring_sem, agx_s, agx_r, agp_s, agp_r, fwd_s, fwd_r, rsd_s, rsd_r, rsi_s, rsi_r):
    rows, width = m_hbm.shape
    ffn = wo_hbm.shape[0]
    me = lax.axis_index("grp")
    partner = {"grp": me + 1 - 2 * lax.rem(me, 2)}
    cross = {"grp": lax.rem(me + 2, 4)}
    full = ffn // FF_BLOCK
    rest = ffn - full * FF_BLOCK
    chunks = width // OUT_COLS

    barrier = pltpu.get_barrier_semaphore()
    for peer in (partner, cross):
        pl.semaphore_signal(barrier, inc=1, device_id=peer, device_id_type=MESH)

    def in_copy(j):
        slot = lax.rem(j, FF_SLOTS)
        return pltpu.make_async_copy(wi_hbm.at[:, pl.ds(pl.multiple_of(j * FF_BLOCK, FF_BLOCK), FF_BLOCK), :],
                                     ring.at[slot], ring_sem.at[slot])

    def rest_copies():
        slot = full % FF_SLOTS
        return [pltpu.make_async_copy(wi_hbm.at[g, pl.ds(full * FF_BLOCK, rest), :],
                                      ring.at[slot, 0, pl.ds(g * rest, rest), :], rest_sem.at[g]) for g in range(2)]

    def out_copy(c):
        slot = lax.rem(c, OUT_SLOTS)
        return pltpu.make_async_copy(wo_hbm.at[:, pl.ds(pl.multiple_of(c * OUT_COLS, OUT_COLS), OUT_COLS)],
                                     oring.at[slot], oring_sem.at[slot])

    m_copy = pltpu.make_async_copy(m_hbm, m_all.at[pl.ds(rows, rows)], m_sem)
    hid_copy = pltpu.make_async_copy(hid_hbm, hid, hid_sem)
    m_copy.start()
    for j in range(FF_SLOTS):
        in_copy(j).start(priority=1)
    out_copy(0).start(priority=1)
    out_copy(1).start(priority=1)
    hid_copy.start(priority=1)
    m_copy.wait()
    pl.semaphore_wait(barrier, 2)

    piece = rows // AG_CHUNKS

    def remote(src, dst, send, recv, peer):
        return pltpu.make_async_remote_copy(src_ref=src, dst_ref=dst, send_sem=send, recv_sem=recv,
                                            device_id=peer, device_id_type=MESH)

    to_cross = [remote(m_all.at[pl.ds(rows + k * piece, piece)], m_all.at[pl.ds(k * piece, piece)],
                       agx_s.at[k], agx_r.at[k], cross) for k in range(AG_CHUNKS)]
    to_partner = remote(m_all.at[pl.ds(rows, rows)], m_all.at[pl.ds(2 * rows, rows)], agp_s, agp_r, partner)
    forward = [remote(m_all.at[pl.ds(k * piece, piece)], m_all.at[pl.ds(3 * rows + k * piece, piece)],
                      fwd_s.at[k], fwd_r.at[k], partner) for k in range(AG_CHUNKS)]

    def swiglu(gate, up):
        return (gate / (1.0 + jnp.exp(-gate)) * up).astype(BF16)

    contract_last = (((1,), (1,)), ((), ()))

    tiles = width // FF_BLOCK

    def gate_up(j):
        slot = lax.rem(j, FF_SLOTS)
        gate = lax.dot_general(m_all[...], ring[slot, 0], contract_last, preferred_element_type=F32)
        up = lax.dot_general(m_all[...], ring[slot, 1], contract_last, preferred_element_type=F32)
        act[:, pl.ds(pl.multiple_of(j * FF_BLOCK, FF_BLOCK), FF_BLOCK)] = swiglu(gate, up)

    def chip_rows(j):
        cols = pl.ds(pl.multiple_of(j * FF_BLOCK, FF_BLOCK), FF_BLOCK)
        left = m_all[pl.ds(rows, 2 * rows), :]
        both = []
        for g in range(2):
            turned = []
            for k in range(tiles):
                tile = ring[j, g, :, pl.ds(k * FF_BLOCK, FF_BLOCK)].T
                ring[j, g, :, pl.ds(k * FF_BLOCK, FF_BLOCK)] = tile
                turned.append(tile)
            both.append(jnp.dot(left, jnp.concatenate(turned, axis=0), preferred_element_type=F32))
        act[pl.ds(rows, 2 * rows), cols] = swiglu(*both)

    def other_rows(j):
        cols = pl.ds(pl.multiple_of(j * FF_BLOCK, FF_BLOCK), FF_BLOCK)
        left = jnp.concatenate([m_all[pl.ds(0, rows), :], m_all[pl.ds(3 * rows, rows), :]], axis=0)
        both = []
        for g in range(2):
            turned = [ring[j, g, :, pl.ds(k * FF_BLOCK, FF_BLOCK)] for k in range(tiles)]
            both.append(jnp.dot(left, jnp.concatenate(turned, axis=0), preferred_element_type=F32))
        result = swiglu(*both)
        act[pl.ds(0, rows), cols] = result[:rows]
        act[pl.ds(3 * rows, rows), cols] = result[rows:]

    for copy in to_cross:
        copy.start()
    to_partner.start()
    to_partner.wait_recv()

    def early(j, carry):
        in_copy(j).wait()
        chip_rows(j)
        for k in range(AG_CHUNKS):
            @pl.when(j == min(2 * k + 2, FF_SLOTS - 1))
            def _():
                to_cross[k].wait_recv()
                forward[k].start()

        return carry

    lax.fori_loop(0, FF_SLOTS, early, 0)
    for k in range(AG_CHUNKS):
        forward[k].wait_recv()

    def late(t, carry):
        for k in range(2):
            other_rows(2 * t + k)
        for k in range(2):
            in_copy(2 * t + k + FF_SLOTS).start(priority=1)
        return carry

    lax.fori_loop(0, FF_SLOTS // 2, late, 0)

    first = FF_SLOTS
    for count in FF_GROUPS:
        for j in range(first, first + count):
            in_copy(j).wait()
        last = first + count == full
        if last:
            for copy in rest_copies():
                copy.wait()
        for j in range(first, first + count):
            gate_up(j)
        if last:
            both = lax.dot_general(m_all[...], ring[full % FF_SLOTS, 0], contract_last, preferred_element_type=F32)
            act[:, pl.ds(full * FF_BLOCK, rest)] = swiglu(both[:, :rest], both[:, rest:])
        for j in range(first, first + count):
            if j + FF_SLOTS < full:
                in_copy(j + FF_SLOTS).start(priority=1)
            elif j + FF_SLOTS == full:
                for copy in rest_copies():
                    copy.start(priority=1)
        if first + FF_SLOTS <= full < first + count + FF_SLOTS:
            for c in range(2, OUT_SLOTS):
                out_copy(c).start(priority=1)
        first += count
    hid_copy.wait()

    def die_copy(c):
        return remote(send_d.at[c], recv_d.at[c], rsd_s.at[c], rsd_r.at[c], partner)

    def chip_copy(c):
        return remote(send_i.at[c], recv_i.at[c], rsi_s.at[c], rsi_r.at[c], cross)

    def finish(c):
        cols = pl.ds(pl.multiple_of(c * OUT_COLS, OUT_COLS), OUT_COLS)
        die_copy(c).wait_recv()
        send_i[c] = (keep[lax.rem(c, 2), pl.ds(0, rows)] + recv_d[c, pl.ds(rows, rows)].astype(F32)).astype(BF16)
        hid[:, cols] += keep[lax.rem(c, 2), pl.ds(rows, rows)] + recv_d[c, pl.ds(0, rows)].astype(F32)
        chip_copy(c).start()

    def down(c, carry):
        out_copy(c).wait()
        part = jnp.dot(act[...], oring[lax.rem(c, OUT_SLOTS)], preferred_element_type=F32)

        @pl.when(c + OUT_SLOTS < chunks)
        def _():
            out_copy(c + OUT_SLOTS).start(priority=1)

        send_d[c] = part[2 * rows:].astype(BF16)
        keep[lax.rem(c, 2)] = part[:2 * rows]
        die_copy(c).start()

        @pl.when(c > 0)
        def _():
            finish(c - 1)

        return carry

    lax.fori_loop(0, chunks, down, 0)
    finish(chunks - 1)
    for c in range(chunks):
        cols = pl.ds(c * OUT_COLS, OUT_COLS)
        chip_copy(c).wait_recv()
        y_ref[:, cols] = (hid[:, cols] + recv_i[c].astype(F32)).astype(BF16)
    for copy in (*to_cross, to_partner, *forward):
        copy.wait_send()
    for c in range(chunks):
        die_copy(c).wait_send()
        chip_copy(c).wait_send()


def solution(mesh):
    row_spec = P(('rep', 'grp'))
    repl_spec = P()
    vmem = pl.BlockSpec(memory_space=pltpu.VMEM)
    hbm = pl.BlockSpec(memory_space=pl.ANY)
    dma = pltpu.SemaphoreType.DMA

    def local_layer(x_in, seq_len, k_cache, v_cache, gamma_attn, w_qkv, b_qkv, w_proj, gamma_mlp, w_in, w_out):
        rows, width = x_in.shape
        cache_len, kv_heads = k_cache.shape[1:3]
        q_heads = w_proj.shape[0] // HEAD
        ffn = w_out.shape[0]
        cache_rows = cache_len * kv_heads

        flat = jax.ShapeDtypeStruct((rows, cache_rows, HEAD), BF16)
        mlp_in, hidden, k_out, v_out = pl.pallas_call(
            functools.partial(attention_kernel, q_heads, kv_heads),
            out_shape=(jax.ShapeDtypeStruct((rows, width), BF16), jax.ShapeDtypeStruct((rows, width), F32), flat, flat),
            in_specs=[hbm] * 9,
            out_specs=(vmem, vmem, hbm, hbm),
            scratch_shapes=[
                pltpu.SMEM((rows,), jnp.int32),
                pltpu.VMEM((rows, width), BF16),
                pltpu.VMEM((width,), BF16),
                pltpu.VMEM((b_qkv.shape[0],), BF16),
                pltpu.VMEM((width,), BF16),
                pltpu.VMEM((QKV_SLOTS, width, QKV_COLS), BF16),
                pltpu.VMEM((SEQ_SLOTS, SEQ_STEP, cache_rows, HEAD), BF16),
                pltpu.VMEM((SEQ_SLOTS, SEQ_STEP, cache_rows, HEAD), BF16),
                pltpu.VMEM((rows, HEAD), F32),
                pltpu.VMEM((rows, width), BF16),
                pltpu.VMEM((rows, HEAD_ROWS, HEAD), F32),
                pltpu.VMEM((rows, 8, HEAD), F32),
                pltpu.VMEM((rows, 8, HEAD), F32),
                pltpu.VMEM((rows, HEAD_ROWS, HEAD), F32),
                dma((5,)), dma((QKV_SLOTS,)), dma((SEQ_SLOTS,)), dma((SEQ_SLOTS,)), dma((SEQ_SLOTS,)), dma((SEQ_SLOTS,)),
            ],
            compiler_params=pltpu.CompilerParams(vmem_limit_bytes=60 * 1024 * 1024),
            name="attention",
        )(seq_len, x_in, gamma_attn, b_qkv, gamma_mlp, w_qkv, w_proj,
          k_cache.reshape(rows, cache_rows, HEAD), v_cache.reshape(rows, cache_rows, HEAD))

        chunks = width // OUT_COLS
        layer_out = pl.pallas_call(
            mlp_kernel,
            out_shape=jax.ShapeDtypeStruct((rows, width), BF16),
            in_specs=[hbm] * 4,
            out_specs=vmem,
            scratch_shapes=[
                pltpu.VMEM((FF_SLOTS, 2, FF_BLOCK, width), BF16),
                pltpu.VMEM((OUT_SLOTS, ffn, OUT_COLS), BF16),
                pltpu.VMEM((4 * rows, width), BF16),
                pltpu.VMEM((rows, width), F32),
                pltpu.VMEM((4 * rows, ffn), BF16),
                pltpu.VMEM((chunks, 2 * rows, OUT_COLS), BF16),
                pltpu.VMEM((chunks, 2 * rows, OUT_COLS), BF16),
                pltpu.VMEM((2, 2 * rows, OUT_COLS), F32),
                pltpu.VMEM((chunks, rows, OUT_COLS), BF16),
                pltpu.VMEM((chunks, rows, OUT_COLS), BF16),
                dma, dma, dma((FF_SLOTS,)), dma((2,)), dma((OUT_SLOTS,)),
                dma((AG_CHUNKS,)), dma((AG_CHUNKS,)), dma, dma, dma((AG_CHUNKS,)), dma((AG_CHUNKS,)),
                dma((chunks,)), dma((chunks,)), dma((chunks,)), dma((chunks,)),
            ],
            compiler_params=pltpu.CompilerParams(collective_id=0, has_side_effects=True,
                                                 vmem_limit_bytes=67043328),
            name="mlp",
        )(mlp_in, hidden, w_in, w_out)
        return layer_out, k_out.reshape(k_cache.shape), v_out.reshape(v_cache.shape)

    return jax.shard_map(local_layer, mesh=mesh,
                         in_specs=(row_spec, row_spec, row_spec, row_spec, repl_spec, repl_spec, repl_spec,
                                   repl_spec, repl_spec, P(None, 'grp', None), P('grp', None)),
                         out_specs=(row_spec, row_spec, row_spec), check_vma=False)
```

```python
import functools
import math

import jax
import jax.numpy as jnp
from jax import lax
from jax.experimental import pallas as pl
from jax.experimental.pallas import tpu as pltpu
from jax.sharding import PartitionSpec as P

HEAD = 128
ROPE_BASE = 10000.0
EPS = 1e-5
MESH = pl.DeviceIdType.MESH
F32 = jnp.float32
BF16 = jnp.bfloat16
LOG2E = 1.4426950408889634

QKV_COLS = 512
QKV_SLOTS = 6
PROJ_AHEAD = 4
SEQ_STEP = 4
SEQ_SLOTS = 4
HEAD_ROWS = 32
FF_BLOCK = 256
FF_SLOTS = 8
OUT_COLS = 512
OUT_SLOTS = 5
AG_CHUNKS = 4


def rms_norm(vals, gain):
    mean_sq = jnp.mean(vals * vals, axis=-1, keepdims=True)
    return (vals * lax.rsqrt(mean_sq + EPS) * gain.astype(F32).reshape(1, -1)).astype(BF16)


def rotary_tables(len_ref, table, rows):
    rot_dim = HEAD // 2
    for b in range(rows):
        table[pl.ds(b, 1), :] = jnp.full((1, HEAD), len_ref[b], jnp.int32).astype(F32)
    dim = lax.broadcasted_iota(jnp.int32, (1, HEAD), 1)
    pair = (dim // 2 * 2).astype(F32)
    inv_freq = jnp.where(dim < rot_dim, jnp.exp(pair * (-math.log(ROPE_BASE) / rot_dim)), 0.0)
    angles = table[...] * inv_freq
    sine = jnp.sin(angles)
    return jnp.cos(angles), jnp.where(lax.rem(dim, 2) == 0, -sine, sine)


def attention_kernel(q_heads, kv_heads, len_hbm, x_hbm, gain_hbm, bias_hbm, gain2_hbm, w_hbm, wp_hbm, k_hbm, v_hbm,
                     m_ref, hid_ref, ko_hbm, vo_hbm,
                     len_ref, x_ref, gain_ref, bias_ref, gain2_ref, wbuf, kbuf, vbuf, table, n_scr, q_scr, kn_scr, vn_scr,
                     ctx_ref, small_sem, w_sem, ki_sem, vi_sem, ko_sem, vo_sem):
    rows, width = x_ref.shape
    blocks = w_hbm.shape[1] // QKV_COLS
    proj_blocks = wp_hbm.shape[1] // QKV_COLS
    steps = rows // SEQ_STEP
    group = q_heads // kv_heads
    heads_per_block = QKV_COLS // HEAD

    def proj_copy(i):
        slot = (blocks + i) % QKV_SLOTS
        return pltpu.make_async_copy(wp_hbm.at[:, pl.ds(i * QKV_COLS, QKV_COLS)], wbuf.at[slot], w_sem.at[slot])

    def w_copy(i):
        return pltpu.make_async_copy(w_hbm.at[:, pl.ds(i * QKV_COLS, QKV_COLS)], wbuf.at[i % QKV_SLOTS],
                                     w_sem.at[i % QKV_SLOTS])

    def in_copies(i):
        slot = lax.rem(i, SEQ_SLOTS)
        part = pl.ds(i * SEQ_STEP, SEQ_STEP)
        return (pltpu.make_async_copy(k_hbm.at[part], kbuf.at[slot], ki_sem.at[slot]),
                pltpu.make_async_copy(v_hbm.at[part], vbuf.at[slot], vi_sem.at[slot]))

    def out_copies(i):
        slot = lax.rem(i, SEQ_SLOTS)
        part = pl.ds(i * SEQ_STEP, SEQ_STEP)
        return (pltpu.make_async_copy(kbuf.at[slot], ko_hbm.at[part], ko_sem.at[slot]),
                pltpu.make_async_copy(vbuf.at[slot], vo_hbm.at[part], vo_sem.at[slot]))

    small = [pltpu.make_async_copy(src, dst, small_sem.at[i]) for i, (src, dst) in enumerate((
        (x_hbm, x_ref), (gain_hbm, gain_ref), (len_hbm, len_ref), (bias_hbm, bias_ref), (gain2_hbm, gain2_ref)))]
    for copy in small:
        copy.start()
    for i in range(QKV_SLOTS):
        w_copy(i).start(priority=1)
    q_scr[:, pl.ds(q_heads, HEAD_ROWS - q_heads), :] = jnp.zeros((rows, HEAD_ROWS - q_heads, HEAD), F32)
    for copy in small:
        copy.wait()
    n_scr[...] = rms_norm(x_ref[...].astype(F32), gain_ref[...])
    even = lax.rem(lax.broadcasted_iota(jnp.int32, (rows, HEAD), 1), 2) == 0
    cosine, sine = rotary_tables(len_ref, table, rows)

    for i in range(blocks):
        w_copy(i).wait()
        part = jnp.dot(n_scr[...], wbuf[i % QKV_SLOTS], preferred_element_type=F32)
        part = part + bias_ref[pl.ds(i * QKV_COLS, QKV_COLS)].astype(F32).reshape(1, -1)
        if i + QKV_SLOTS < blocks:
            w_copy(i + QKV_SLOTS).start(priority=1)
        elif i + QKV_SLOTS < blocks + PROJ_AHEAD:
            proj_copy(i + QKV_SLOTS - blocks).start(priority=1)
        if i >= blocks - 4 and i < blocks - 2:
            for copy in in_copies(i + 4 - blocks):
                copy.start()
        for j in range(heads_per_block):
            head = i * heads_per_block + j
            vals = part[:, j * HEAD:(j + 1) * HEAD]
            if head < q_heads + kv_heads:
                other = jnp.where(even, pltpu.roll(vals, HEAD - 1, 1), pltpu.roll(vals, 1, 1))
                vals = vals * cosine + other * sine
            if head < q_heads:
                q_scr[:, head, :] = vals
            elif head < q_heads + kv_heads:
                for rep in range(8 // kv_heads):
                    kn_scr[:, rep * kv_heads + head - q_heads, :] = vals
            else:
                for rep in range(8 // kv_heads):
                    vn_scr[:, rep * kv_heads + head - q_heads - kv_heads, :] = vals

    cols = kbuf.shape[2]
    col = lax.broadcasted_iota(jnp.int32, (HEAD_ROWS, cols), 1)
    row_group = jnp.minimum(lax.broadcasted_iota(jnp.int32, (HEAD_ROWS, cols), 0) // group, kv_heads - 1)
    own_group = lax.rem(col, kv_heads) == row_group
    positions = 16 // kv_heads

    def attend(i, carry):
        slot = lax.rem(i, SEQ_SLOTS)

        @pl.when(i >= 2)
        def _():
            for copy in out_copies(i - 2):
                copy.wait()

        @pl.when(i + 2 < steps)
        def _():
            for copy in in_copies(i + 2):
                copy.start()

        for copy in in_copies(i):
            copy.wait()
        lengths = [len_ref[i * SEQ_STEP + s] for s in range(SEQ_STEP)]
        new_row = lax.broadcasted_iota(jnp.int32, (16, HEAD), 0) // kv_heads
        for s in range(SEQ_STEP):
            base = pl.multiple_of((lengths[s] // positions) * 16, 16)
            hit = new_row == lax.rem(lengths[s], positions)
            for buf, new in ((kbuf, kn_scr), (vbuf, vn_scr)):
                fresh = new[i * SEQ_STEP + s]
                fresh = jnp.concatenate([fresh, fresh], axis=0).astype(BF16).astype(F32)
                old = buf[slot, s, pl.ds(base, 16), :].astype(F32)
                buf[slot, s, pl.ds(base, 16), :] = jnp.where(hit, fresh, old).astype(BF16)
        scores = [lax.dot_general(q_scr[i * SEQ_STEP + s].astype(BF16), kbuf[slot, s], (((1,), (1,)), ((), ())),
                                  preferred_element_type=F32) for s in range(SEQ_STEP)]
        for s in range(SEQ_STEP):
            seen = jnp.logical_and(own_group, col < (lengths[s] + 1) * kv_heads)
            logits = jnp.where(seen, scores[s] * (HEAD ** -0.5 * LOG2E), -jnp.inf)
            top = jnp.max(logits, axis=-1, keepdims=True)
            weights = jnp.exp2(logits - top)
            total = jnp.sum(weights, axis=-1, keepdims=True)
            probs = (weights * (1.0 / total)).astype(BF16)
            ctx_ref[i * SEQ_STEP + s] = jnp.dot(probs, vbuf[slot, s], preferred_element_type=F32)
        for copy in out_copies(i):
            copy.start()

        @pl.when(lax.rem(i + 1, 16 // SEQ_STEP) == 0)
        def _():
            part = pl.ds(pl.multiple_of((i + 1) * SEQ_STEP - 16, 16), 16)
            for head in range(q_heads):
                n_scr[part, pl.ds(head * HEAD, HEAD)] = ctx_ref[part, head, :].astype(BF16)

        for n in range(PROJ_AHEAD, QKV_SLOTS):
            @pl.when(i == steps - 1 - QKV_SLOTS + n)
            def _():
                proj_copy(n).start(priority=1)

        return carry

    lax.fori_loop(0, steps, attend, 0)
    for i in range(proj_blocks):
        cols = pl.ds(i * QKV_COLS, QKV_COLS)
        proj_copy(i).wait()
        part = jnp.dot(n_scr[...], wbuf[(blocks + i) % QKV_SLOTS], preferred_element_type=F32)
        if i + QKV_SLOTS < proj_blocks:
            proj_copy(i + QKV_SLOTS).start(priority=1)
        hid_ref[:, cols] = x_ref[:, cols].astype(F32) + part
    m_ref[...] = rms_norm(hid_ref[...], gain2_ref[...])
    for i in (steps - 2, steps - 1):
        for copy in out_copies(i):
            copy.wait()


def mlp_kernel(m_hbm, hid_hbm, wi_hbm, wo_hbm, y_ref,
               ring, rest_buf, oring, m_all, hid, act, send_d, recv_d, keep, send_i, recv_i,
               m_sem, hid_sem, ring_sem, rest_sem, oring_sem, agx_s, agx_r, agp_s, agp_r, fwd_s, fwd_r, rsd_s, rsd_r, rsi_s, rsi_r):
    rows, width = m_hbm.shape
    ffn = wo_hbm.shape[0]
    me = lax.axis_index("grp")
    partner = {"grp": me + 1 - 2 * lax.rem(me, 2)}
    cross = {"grp": lax.rem(me + 2, 4)}
    full = ffn // FF_BLOCK
    rest = ffn - full * FF_BLOCK
    chunks = width // OUT_COLS

    barrier = pltpu.get_barrier_semaphore()
    for peer in (partner, cross):
        pl.semaphore_signal(barrier, inc=1, device_id=peer, device_id_type=MESH)

    def in_copy(j):
        slot = lax.rem(j, FF_SLOTS)
        return pltpu.make_async_copy(wi_hbm.at[:, pl.ds(pl.multiple_of(j * FF_BLOCK, FF_BLOCK), FF_BLOCK), :],
                                     ring.at[slot], ring_sem.at[slot])

    rest_copies = [pltpu.make_async_copy(wi_hbm.at[g, pl.ds(full * FF_BLOCK, rest), :],
                                         rest_buf.at[pl.ds(g * rest, rest), :], rest_sem.at[g]) for g in range(2)]

    def out_copy(c):
        slot = lax.rem(c, OUT_SLOTS)
        return pltpu.make_async_copy(wo_hbm.at[:, pl.ds(pl.multiple_of(c * OUT_COLS, OUT_COLS), OUT_COLS)],
                                     oring.at[slot], oring_sem.at[slot])

    m_copy = pltpu.make_async_copy(m_hbm, m_all.at[pl.ds(rows, rows)], m_sem)
    hid_copy = pltpu.make_async_copy(hid_hbm, hid, hid_sem)
    m_copy.start()
    for j in range(FF_SLOTS):
        in_copy(j).start(priority=1)
    hid_copy.start(priority=1)
    m_copy.wait()
    pl.semaphore_wait(barrier, 2)

    piece = rows // AG_CHUNKS

    def remote(src, dst, send, recv, peer):
        return pltpu.make_async_remote_copy(src_ref=src, dst_ref=dst, send_sem=send, recv_sem=recv,
                                            device_id=peer, device_id_type=MESH)

    to_cross = [remote(m_all.at[pl.ds(rows + k * piece, piece)], m_all.at[pl.ds(k * piece, piece)],
                       agx_s.at[k], agx_r.at[k], cross) for k in range(AG_CHUNKS)]
    to_partner = remote(m_all.at[pl.ds(rows, rows)], m_all.at[pl.ds(2 * rows, rows)], agp_s, agp_r, partner)
    forward = [remote(m_all.at[pl.ds(k * piece, piece)], m_all.at[pl.ds(3 * rows + k * piece, piece)],
                      fwd_s.at[k], fwd_r.at[k], partner) for k in range(AG_CHUNKS)]

    def swiglu(gate, up):
        return (gate / (1.0 + jnp.exp(-gate)) * up).astype(BF16)

    contract_last = (((1,), (1,)), ((), ()))

    tiles = width // FF_BLOCK

    def gate_up(j):
        slot = lax.rem(j, FF_SLOTS)
        gate = lax.dot_general(m_all[...], ring[slot, 0], contract_last, preferred_element_type=F32)
        up = lax.dot_general(m_all[...], ring[slot, 1], contract_last, preferred_element_type=F32)
        act[:, pl.ds(pl.multiple_of(j * FF_BLOCK, FF_BLOCK), FF_BLOCK)] = swiglu(gate, up)

    def transpose_tiles(ref):
        tiles = []
        for k in range(width // FF_BLOCK):
            tile = ref[:, pl.ds(k * FF_BLOCK, FF_BLOCK)].T
            ref[:, pl.ds(k * FF_BLOCK, FF_BLOCK)] = tile
            tiles.append(tile)
        return jnp.concatenate(tiles, axis=0)

    def transposed_tiles(ref):
        return jnp.concatenate([ref[:, pl.ds(k * FF_BLOCK, FF_BLOCK)] for k in range(width // FF_BLOCK)], axis=0)

    def chip_rows():
        return m_all[pl.ds(rows, 2 * rows), :]

    def other_rows():
        return jnp.concatenate([m_all[pl.ds(0, rows), :], m_all[pl.ds(3 * rows, rows), :]], axis=0)

    def store_chip(cols, result):
        act[pl.ds(rows, 2 * rows), cols] = result

    def store_other(cols, result):
        act[pl.ds(0, rows), cols] = result[:rows]
        act[pl.ds(3 * rows, rows), cols] = result[rows:]

    def half_rows(j, tiles, left, store):
        gate, up = (jnp.dot(left(), tiles(ring.at[j, g]), preferred_element_type=F32) for g in range(2))
        store(pl.ds(pl.multiple_of(j * FF_BLOCK, FF_BLOCK), FF_BLOCK), swiglu(gate, up))

    def half_rows_rest(tiles, left, store):
        both = jnp.dot(left(), tiles(rest_buf), preferred_element_type=F32)
        store(pl.ds(full * FF_BLOCK, rest), swiglu(both[:, :rest], both[:, rest:]))

    for copy in to_cross:
        copy.start()
    to_partner.start()
    to_partner.wait_recv()

    def early(j, carry):
        in_copy(j).wait()
        half_rows(j, transpose_tiles, chip_rows, store_chip)

        @pl.when(j == 1)
        def _():
            for copy in rest_copies:
                copy.start(priority=1)

        for c in range(2):
            @pl.when(j == 2 * c + 2)
            def _():
                out_copy(c).start(priority=1)

        for k in range(AG_CHUNKS - 1):
            @pl.when(j == 2 * k + 2)
            def _():
                to_cross[k].wait_recv()
                forward[k].start()

        return carry

    lax.fori_loop(0, FF_SLOTS, early, 0)
    for copy in rest_copies:
        copy.wait()
    half_rows_rest(transpose_tiles, chip_rows, store_chip)
    to_cross[AG_CHUNKS - 1].wait_recv()
    forward[AG_CHUNKS - 1].start()
    for k in range(AG_CHUNKS):
        forward[k].wait_recv()

    def late(t, carry):
        for k in range(2):
            half_rows(2 * t + k, transposed_tiles, other_rows, store_other)
        for k in range(2):
            in_copy(2 * t + k + FF_SLOTS).start(priority=1)
        return carry

    lax.fori_loop(0, FF_SLOTS // 2, late, 0)
    half_rows_rest(transposed_tiles, other_rows, store_other)

    def main(t, carry):
        for k in range(2):
            in_copy(FF_SLOTS + 2 * t + k).wait()
        for k in range(2):
            gate_up(FF_SLOTS + 2 * t + k)

        @pl.when(t == 0)
        def _():
            for j in range(2 * FF_SLOTS, full):
                in_copy(j).start(priority=1)

        for c in range(2, OUT_SLOTS):
            @pl.when(t == c)
            def _():
                out_copy(c).start(priority=1)

        return carry

    lax.fori_loop(0, (full - FF_SLOTS) // 2, main, 0)
    hid_copy.wait()

    def die_copy(c):
        return remote(send_d.at[c], recv_d.at[c], rsd_s.at[c], rsd_r.at[c], partner)

    def chip_copy(c):
        return remote(send_i.at[c], recv_i.at[c], rsi_s.at[c], rsi_r.at[c], cross)

    def finish(c):
        cols = pl.ds(pl.multiple_of(c * OUT_COLS, OUT_COLS), OUT_COLS)
        die_copy(c).wait_recv()
        send_i[c] = (keep[lax.rem(c, 2), pl.ds(0, rows)] + recv_d[c, pl.ds(rows, rows)].astype(F32)).astype(BF16)
        hid[:, cols] += keep[lax.rem(c, 2), pl.ds(rows, rows)] + recv_d[c, pl.ds(0, rows)].astype(F32)
        chip_copy(c).start()

    def down(c, carry):
        out_copy(c).wait()
        part = jnp.dot(act[...], oring[lax.rem(c, OUT_SLOTS)], preferred_element_type=F32)

        @pl.when(c + OUT_SLOTS < chunks)
        def _():
            out_copy(c + OUT_SLOTS).start(priority=1)

        send_d[c] = part[2 * rows:].astype(BF16)
        keep[lax.rem(c, 2)] = part[:2 * rows]
        die_copy(c).start()

        @pl.when(c > 0)
        def _():
            finish(c - 1)

        return carry

    lax.fori_loop(0, chunks, down, 0)
    finish(chunks - 1)
    for c in range(chunks):
        cols = pl.ds(c * OUT_COLS, OUT_COLS)
        chip_copy(c).wait_recv()
        y_ref[:, cols] = (hid[:, cols] + recv_i[c].astype(F32)).astype(BF16)
    for copy in (*to_cross, to_partner, *forward):
        copy.wait_send()
    for c in range(chunks):
        die_copy(c).wait_send()
        chip_copy(c).wait_send()


def solution(mesh):
    row_spec = P(('rep', 'grp'))
    repl_spec = P()
    vmem = pl.BlockSpec(memory_space=pltpu.VMEM)
    hbm = pl.BlockSpec(memory_space=pl.ANY)
    dma = pltpu.SemaphoreType.DMA

    def local_layer(x_in, seq_len, k_cache, v_cache, gamma_attn, w_qkv, b_qkv, w_proj, gamma_mlp, w_in, w_out):
        rows, width = x_in.shape
        cache_len, kv_heads = k_cache.shape[1:3]
        q_heads = w_proj.shape[0] // HEAD
        ffn = w_out.shape[0]
        cache_rows = cache_len * kv_heads

        flat = jax.ShapeDtypeStruct((rows, cache_rows, HEAD), BF16)
        mlp_in, hidden, k_out, v_out = pl.pallas_call(
            functools.partial(attention_kernel, q_heads, kv_heads),
            out_shape=(jax.ShapeDtypeStruct((rows, width), BF16), jax.ShapeDtypeStruct((rows, width), F32), flat, flat),
            in_specs=[hbm] * 9,
            out_specs=(vmem, vmem, hbm, hbm),
            scratch_shapes=[
                pltpu.SMEM((rows,), jnp.int32),
                pltpu.VMEM((rows, width), BF16),
                pltpu.VMEM((width,), BF16),
                pltpu.VMEM((b_qkv.shape[0],), BF16),
                pltpu.VMEM((width,), BF16),
                pltpu.VMEM((QKV_SLOTS, width, QKV_COLS), BF16),
                pltpu.VMEM((SEQ_SLOTS, SEQ_STEP, cache_rows, HEAD), BF16),
                pltpu.VMEM((SEQ_SLOTS, SEQ_STEP, cache_rows, HEAD), BF16),
                pltpu.VMEM((rows, HEAD), F32),
                pltpu.VMEM((rows, width), BF16),
                pltpu.VMEM((rows, HEAD_ROWS, HEAD), F32),
                pltpu.VMEM((rows, 8, HEAD), F32),
                pltpu.VMEM((rows, 8, HEAD), F32),
                pltpu.VMEM((rows, HEAD_ROWS, HEAD), F32),
                dma((5,)), dma((QKV_SLOTS,)), dma((SEQ_SLOTS,)), dma((SEQ_SLOTS,)), dma((SEQ_SLOTS,)), dma((SEQ_SLOTS,)),
            ],
            compiler_params=pltpu.CompilerParams(vmem_limit_bytes=60 * 1024 * 1024),
            name="attention",
        )(seq_len, x_in, gamma_attn, b_qkv, gamma_mlp, w_qkv, w_proj,
          k_cache.reshape(rows, cache_rows, HEAD), v_cache.reshape(rows, cache_rows, HEAD))

        chunks = width // OUT_COLS
        layer_out = pl.pallas_call(
            mlp_kernel,
            out_shape=jax.ShapeDtypeStruct((rows, width), BF16),
            in_specs=[hbm] * 4,
            out_specs=vmem,
            scratch_shapes=[
                pltpu.VMEM((FF_SLOTS, 2, FF_BLOCK, width), BF16),
                pltpu.VMEM((FF_BLOCK, width), BF16),
                pltpu.VMEM((OUT_SLOTS, ffn, OUT_COLS), BF16),
                pltpu.VMEM((4 * rows, width), BF16),
                pltpu.VMEM((rows, width), F32),
                pltpu.VMEM((4 * rows, ffn), BF16),
                pltpu.VMEM((chunks, 2 * rows, OUT_COLS), BF16),
                pltpu.VMEM((chunks, 2 * rows, OUT_COLS), BF16),
                pltpu.VMEM((2, 2 * rows, OUT_COLS), F32),
                pltpu.VMEM((chunks, rows, OUT_COLS), BF16),
                pltpu.VMEM((chunks, rows, OUT_COLS), BF16),
                dma, dma, dma((FF_SLOTS,)), dma((2,)), dma((OUT_SLOTS,)),
                dma((AG_CHUNKS,)), dma((AG_CHUNKS,)), dma, dma, dma((AG_CHUNKS,)), dma((AG_CHUNKS,)),
                dma((chunks,)), dma((chunks,)), dma((chunks,)), dma((chunks,)),
            ],
            compiler_params=pltpu.CompilerParams(collective_id=0, has_side_effects=True,
                                                 vmem_limit_bytes=67043328),
            name="mlp",
        )(mlp_in, hidden, w_in, w_out)
        return layer_out, k_out.reshape(k_cache.shape), v_out.reshape(v_cache.shape)

    return jax.shard_map(local_layer, mesh=mesh,
                         in_specs=(row_spec, row_spec, row_spec, row_spec, repl_spec, repl_spec, repl_spec,
                                   repl_spec, repl_spec, P(None, 'grp', None), P('grp', None)),
                         out_specs=(row_spec, row_spec, row_spec), check_vma=False)
```

```python
import functools
import math

import jax
import jax.numpy as jnp
from jax import lax
from jax.experimental import pallas as pl
from jax.experimental.pallas import tpu as pltpu
from jax.sharding import PartitionSpec as P

HEAD = 128
ROPE_BASE = 10000.0
EPS = 1e-5
MESH = pl.DeviceIdType.MESH
F32 = jnp.float32
BF16 = jnp.bfloat16
LOG2E = 1.4426950408889634

QKV_COLS = 512
QKV_SLOTS = 7
PROJ_GROUP = 2
PROJ_AHEAD = 3
SEQ_STEP = 8
SEQ_SLOTS = 4
HEAD_ROWS = 32
FF_BLOCK = 256
FF_SLOTS = 8
OUT_COLS = 512
OUT_SLOTS = 5
AG_CHUNKS = 4


def rms_norm(vals, gain):
    mean_sq = jnp.mean(vals * vals, axis=-1, keepdims=True)
    return (vals * lax.rsqrt(mean_sq + EPS) * gain.astype(F32).reshape(1, -1)).astype(BF16)


def rotary_tables(len_ref, table, rows):
    rot_dim = HEAD // 2
    for b in range(rows):
        table[pl.ds(b, 1), :] = jnp.full((1, HEAD), len_ref[b], jnp.int32).astype(F32)
    dim = lax.broadcasted_iota(jnp.int32, (1, HEAD), 1)
    pair = (dim // 2 * 2).astype(F32)
    inv_freq = jnp.where(dim < rot_dim, jnp.exp(pair * (-math.log(ROPE_BASE) / rot_dim)), 0.0)
    angles = table[...] * inv_freq
    sine = jnp.sin(angles)
    return jnp.cos(angles), jnp.where(lax.rem(dim, 2) == 0, -sine, sine)


def attention_kernel(q_heads, kv_heads, len_hbm, x_hbm, gain_hbm, bias_hbm, gain2_hbm, w_hbm, wp_hbm, k_hbm, v_hbm,
                     m_ref, hid_ref, ko_hbm, vo_hbm,
                     len_ref, x_ref, gain_ref, bias_ref, gain2_ref, wbuf, kbuf, vbuf, table, n_scr, q_scr, kn_scr, vn_scr,
                     ctx_ref, small_sem, w_sem, ki_sem, vi_sem, ko_sem, vo_sem):
    rows, width = x_ref.shape
    blocks = w_hbm.shape[1] // QKV_COLS
    proj_blocks = wp_hbm.shape[1] // QKV_COLS
    steps = rows // SEQ_STEP
    group = q_heads // kv_heads
    heads_per_block = QKV_COLS // HEAD

    def proj_copy(i):
        slot = (blocks + i) % QKV_SLOTS
        return pltpu.make_async_copy(wp_hbm.at[:, pl.ds(i * QKV_COLS, QKV_COLS)], wbuf.at[slot], w_sem.at[slot])

    def w_copy(i):
        return pltpu.make_async_copy(w_hbm.at[:, pl.ds(i * QKV_COLS, QKV_COLS)], wbuf.at[i % QKV_SLOTS],
                                     w_sem.at[i % QKV_SLOTS])

    def in_copies(i):
        slot = lax.rem(i, SEQ_SLOTS)
        part = pl.ds(i * SEQ_STEP, SEQ_STEP)
        return (pltpu.make_async_copy(k_hbm.at[part], kbuf.at[slot], ki_sem.at[slot]),
                pltpu.make_async_copy(v_hbm.at[part], vbuf.at[slot], vi_sem.at[slot]))

    def out_copies(i):
        slot = lax.rem(i, SEQ_SLOTS)
        part = pl.ds(i * SEQ_STEP, SEQ_STEP)
        return (pltpu.make_async_copy(kbuf.at[slot], ko_hbm.at[part], ko_sem.at[slot]),
                pltpu.make_async_copy(vbuf.at[slot], vo_hbm.at[part], vo_sem.at[slot]))

    small = [pltpu.make_async_copy(src, dst, small_sem.at[i]) for i, (src, dst) in enumerate((
        (x_hbm, x_ref), (gain_hbm, gain_ref), (len_hbm, len_ref), (bias_hbm, bias_ref), (gain2_hbm, gain2_ref)))]
    for copy in small:
        copy.start()
    for i in range(QKV_SLOTS):
        w_copy(i).start(priority=1)
    q_scr[:, pl.ds(q_heads, HEAD_ROWS - q_heads), :] = jnp.zeros((rows, HEAD_ROWS - q_heads, HEAD), F32)
    for copy in small:
        copy.wait()
    n_scr[...] = rms_norm(x_ref[...].astype(F32), gain_ref[...])
    even = lax.rem(lax.broadcasted_iota(jnp.int32, (rows, HEAD), 1), 2) == 0
    cosine, sine = rotary_tables(len_ref, table, rows)

    for i in range(blocks):
        w_copy(i).wait()
        part = jnp.dot(n_scr[...], wbuf[i % QKV_SLOTS], preferred_element_type=F32)
        part = part + bias_ref[pl.ds(i * QKV_COLS, QKV_COLS)].astype(F32).reshape(1, -1)
        if i + QKV_SLOTS < blocks:
            w_copy(i + QKV_SLOTS).start(priority=1)
        elif i + QKV_SLOTS < blocks + PROJ_AHEAD:
            proj_copy(i + QKV_SLOTS - blocks).start(priority=1)
        if i >= blocks - 4 and i < blocks - 2:
            for copy in in_copies(i + 4 - blocks):
                copy.start()
        for j in range(heads_per_block):
            head = i * heads_per_block + j
            vals = part[:, j * HEAD:(j + 1) * HEAD]
            if head < q_heads + kv_heads:
                other = jnp.where(even, pltpu.roll(vals, HEAD - 1, 1), pltpu.roll(vals, 1, 1))
                vals = vals * cosine + other * sine
            if head < q_heads:
                q_scr[:, head, :] = vals
            elif head < q_heads + kv_heads:
                for rep in range(8 // kv_heads):
                    kn_scr[:, rep * kv_heads + head - q_heads, :] = vals
            else:
                for rep in range(8 // kv_heads):
                    vn_scr[:, rep * kv_heads + head - q_heads - kv_heads, :] = vals

    cols = kbuf.shape[2]
    col = lax.broadcasted_iota(jnp.int32, (HEAD_ROWS, cols), 1)
    row_group = jnp.minimum(lax.broadcasted_iota(jnp.int32, (HEAD_ROWS, cols), 0) // group, kv_heads - 1)
    own_group = lax.rem(col, kv_heads) == row_group
    positions = 16 // kv_heads

    def attend(i, carry):
        slot = lax.rem(i, SEQ_SLOTS)

        @pl.when(i >= 2)
        def _():
            for copy in out_copies(i - 2):
                copy.wait()

        @pl.when(i + 2 < steps)
        def _():
            for copy in in_copies(i + 2):
                copy.start()

        for copy in in_copies(i):
            copy.wait()
        lengths = [len_ref[i * SEQ_STEP + s] for s in range(SEQ_STEP)]
        new_row = lax.broadcasted_iota(jnp.int32, (16, HEAD), 0) // kv_heads
        for s in range(SEQ_STEP):
            base = pl.multiple_of((lengths[s] // positions) * 16, 16)
            hit = new_row == lax.rem(lengths[s], positions)
            for buf, new in ((kbuf, kn_scr), (vbuf, vn_scr)):
                fresh = new[i * SEQ_STEP + s]
                fresh = jnp.concatenate([fresh, fresh], axis=0).astype(BF16).astype(F32)
                old = buf[slot, s, pl.ds(base, 16), :].astype(F32)
                buf[slot, s, pl.ds(base, 16), :] = jnp.where(hit, fresh, old).astype(BF16)
        scores = [lax.dot_general(q_scr[i * SEQ_STEP + s].astype(BF16), kbuf[slot, s], (((1,), (1,)), ((), ())),
                                  preferred_element_type=F32) for s in range(SEQ_STEP)]
        for s in range(SEQ_STEP):
            seen = jnp.logical_and(own_group, col < (lengths[s] + 1) * kv_heads)
            logits = jnp.where(seen, scores[s] * (HEAD ** -0.5 * LOG2E), -jnp.inf)
            top = jnp.max(logits, axis=-1, keepdims=True)
            weights = jnp.exp2(logits - top)
            total = jnp.sum(weights, axis=-1, keepdims=True)
            probs = (weights * (1.0 / total)).astype(BF16)
            ctx_ref[i * SEQ_STEP + s] = jnp.dot(probs, vbuf[slot, s], preferred_element_type=F32)
        for copy in out_copies(i):
            copy.start()

        @pl.when(lax.rem(i + 1, 16 // SEQ_STEP) == 0)
        def _():
            part = pl.ds(pl.multiple_of((i + 1) * SEQ_STEP - 16, 16), 16)
            for head in range(q_heads):
                n_scr[part, pl.ds(head * HEAD, HEAD)] = ctx_ref[part, head, :].astype(BF16)

        for n in range(PROJ_AHEAD, QKV_SLOTS):
            @pl.when(i == steps - 1 - (QKV_SLOTS - n) // 2)
            def _():
                proj_copy(n).start(priority=1)

        return carry

    lax.fori_loop(0, steps, attend, 0)
    for first in range(0, proj_blocks, PROJ_GROUP):
        group_blocks = range(first, min(first + PROJ_GROUP, proj_blocks))
        for i in group_blocks:
            proj_copy(i).wait()
        parts = [jnp.dot(n_scr[...], wbuf[(blocks + i) % QKV_SLOTS], preferred_element_type=F32) for i in group_blocks]
        for i in group_blocks:
            if i + QKV_SLOTS < proj_blocks:
                proj_copy(i + QKV_SLOTS).start(priority=1)
            cols = pl.ds(i * QKV_COLS, QKV_COLS)
            hid_ref[:, cols] = x_ref[:, cols].astype(F32) + parts[i - first]
    m_ref[...] = rms_norm(hid_ref[...], gain2_ref[...])
    for i in (steps - 2, steps - 1):
        for copy in out_copies(i):
            copy.wait()


def mlp_kernel(m_hbm, hid_hbm, wi_hbm, wo_hbm, y_ref,
               ring, rest_buf, oring, m_all, hid, act, send_d, recv_d, keep, send_i, recv_i,
               m_sem, hid_sem, ring_sem, rest_sem, oring_sem, agx_s, agx_r, agp_s, agp_r, fwd_s, fwd_r, rsd_s, rsd_r, rsi_s, rsi_r):
    rows, width = m_hbm.shape
    ffn = wo_hbm.shape[0]
    me = lax.axis_index("grp")
    partner = {"grp": me + 1 - 2 * lax.rem(me, 2)}
    cross = {"grp": lax.rem(me + 2, 4)}
    full = ffn // FF_BLOCK
    rest = ffn - full * FF_BLOCK
    chunks = width // OUT_COLS

    barrier = pltpu.get_barrier_semaphore()
    for peer in (partner, cross):
        pl.semaphore_signal(barrier, inc=1, device_id=peer, device_id_type=MESH)

    def in_copy(j):
        slot = lax.rem(j, FF_SLOTS)
        return pltpu.make_async_copy(wi_hbm.at[:, pl.ds(pl.multiple_of(j * FF_BLOCK, FF_BLOCK), FF_BLOCK), :],
                                     ring.at[slot], ring_sem.at[slot])

    rest_copies = [pltpu.make_async_copy(wi_hbm.at[g, pl.ds(full * FF_BLOCK, rest), :],
                                         rest_buf.at[pl.ds(g * rest, rest), :], rest_sem.at[g]) for g in range(2)]

    def out_copy(c):
        slot = lax.rem(c, OUT_SLOTS)
        return pltpu.make_async_copy(wo_hbm.at[:, pl.ds(pl.multiple_of(c * OUT_COLS, OUT_COLS), OUT_COLS)],
                                     oring.at[slot], oring_sem.at[slot])

    m_copy = pltpu.make_async_copy(m_hbm, m_all.at[pl.ds(rows, rows)], m_sem)
    hid_copy = pltpu.make_async_copy(hid_hbm, hid, hid_sem)
    m_copy.start()
    for j in range(FF_SLOTS):
        in_copy(j).start(priority=1)
    hid_copy.start(priority=1)
    m_copy.wait()
    pl.semaphore_wait(barrier, 2)

    piece = rows // AG_CHUNKS

    def remote(src, dst, send, recv, peer):
        return pltpu.make_async_remote_copy(src_ref=src, dst_ref=dst, send_sem=send, recv_sem=recv,
                                            device_id=peer, device_id_type=MESH)

    to_cross = [remote(m_all.at[pl.ds(rows + k * piece, piece)], m_all.at[pl.ds(k * piece, piece)],
                       agx_s.at[k], agx_r.at[k], cross) for k in range(AG_CHUNKS)]
    to_partner = remote(m_all.at[pl.ds(rows, rows)], m_all.at[pl.ds(2 * rows, rows)], agp_s, agp_r, partner)
    forward = [remote(m_all.at[pl.ds(k * piece, piece)], m_all.at[pl.ds(3 * rows + k * piece, piece)],
                      fwd_s.at[k], fwd_r.at[k], partner) for k in range(AG_CHUNKS)]

    def swiglu(gate, up):
        return (gate / (1.0 + jnp.exp(-gate)) * up).astype(BF16)

    contract_last = (((1,), (1,)), ((), ()))

    tiles = width // FF_BLOCK

    def gate_up(j):
        slot = lax.rem(j, FF_SLOTS)
        gate = lax.dot_general(m_all[...], ring[slot, 0], contract_last, preferred_element_type=F32)
        up = lax.dot_general(m_all[...], ring[slot, 1], contract_last, preferred_element_type=F32)
        act[:, pl.ds(pl.multiple_of(j * FF_BLOCK, FF_BLOCK), FF_BLOCK)] = swiglu(gate, up)

    def transpose_tiles(ref):
        tiles = []
        for k in range(width // FF_BLOCK):
            tile = ref[:, pl.ds(k * FF_BLOCK, FF_BLOCK)].T
            ref[:, pl.ds(k * FF_BLOCK, FF_BLOCK)] = tile
            tiles.append(tile)
        return jnp.concatenate(tiles, axis=0)

    def transposed_tiles(ref):
        return jnp.concatenate([ref[:, pl.ds(k * FF_BLOCK, FF_BLOCK)] for k in range(width // FF_BLOCK)], axis=0)

    def chip_rows():
        return m_all[pl.ds(rows, 2 * rows), :]

    def other_rows():
        return jnp.concatenate([m_all[pl.ds(0, rows), :], m_all[pl.ds(3 * rows, rows), :]], axis=0)

    def store_chip(cols, result):
        act[pl.ds(rows, 2 * rows), cols] = result

    def store_other(cols, result):
        act[pl.ds(0, rows), cols] = result[:rows]
        act[pl.ds(3 * rows, rows), cols] = result[rows:]

    def half_rows(j, tiles, left, store):
        gate, up = (jnp.dot(left(), tiles(ring.at[j, g]), preferred_element_type=F32) for g in range(2))
        store(pl.ds(pl.multiple_of(j * FF_BLOCK, FF_BLOCK), FF_BLOCK), swiglu(gate, up))

    def half_rows_rest(tiles, left, store):
        both = jnp.dot(left(), tiles(rest_buf), preferred_element_type=F32)
        store(pl.ds(full * FF_BLOCK, rest), swiglu(both[:, :rest], both[:, rest:]))

    for copy in to_cross:
        copy.start()
    to_partner.start()
    to_partner.wait_recv()

    def early(j, carry):
        in_copy(j).wait()
        half_rows(j, transpose_tiles, chip_rows, store_chip)

        @pl.when(j == 1)
        def _():
            for copy in rest_copies:
                copy.start(priority=1)

        for c in range(2):
            @pl.when(j == 2 * c + 2)
            def _():
                out_copy(c).start(priority=1)

        for k in range(AG_CHUNKS - 1):
            @pl.when(j == 2 * k + 2)
            def _():
                to_cross[k].wait_recv()
                forward[k].start()

        return carry

    lax.fori_loop(0, FF_SLOTS, early, 0)
    for copy in rest_copies:
        copy.wait()
    half_rows_rest(transpose_tiles, chip_rows, store_chip)
    to_cross[AG_CHUNKS - 1].wait_recv()
    forward[AG_CHUNKS - 1].start()
    for k in range(AG_CHUNKS):
        forward[k].wait_recv()

    def late(t, carry):
        for k in range(2):
            half_rows(2 * t + k, transposed_tiles, other_rows, store_other)
        for k in range(2):
            in_copy(2 * t + k + FF_SLOTS).start(priority=1)
        return carry

    lax.fori_loop(0, FF_SLOTS // 2, late, 0)
    half_rows_rest(transposed_tiles, other_rows, store_other)

    def main(t, carry):
        for k in range(2):
            in_copy(FF_SLOTS + 2 * t + k).wait()
        for k in range(2):
            gate_up(FF_SLOTS + 2 * t + k)

        @pl.when(t == 0)
        def _():
            for j in range(2 * FF_SLOTS, full):
                in_copy(j).start(priority=1)

        for c in range(2, OUT_SLOTS):
            @pl.when(t == c)
            def _():
                out_copy(c).start(priority=1)

        return carry

    lax.fori_loop(0, (full - FF_SLOTS) // 2, main, 0)
    hid_copy.wait()

    def die_copy(c):
        return remote(send_d.at[c], recv_d.at[c], rsd_s.at[c], rsd_r.at[c], partner)

    def chip_copy(c):
        return remote(send_i.at[c], recv_i.at[c], rsi_s.at[c], rsi_r.at[c], cross)

    def finish(c):
        cols = pl.ds(pl.multiple_of(c * OUT_COLS, OUT_COLS), OUT_COLS)
        die_copy(c).wait_recv()
        send_i[c] = (keep[lax.rem(c, 2), pl.ds(0, rows)] + recv_d[c, pl.ds(rows, rows)].astype(F32)).astype(BF16)
        hid[:, cols] += keep[lax.rem(c, 2), pl.ds(rows, rows)] + recv_d[c, pl.ds(0, rows)].astype(F32)
        chip_copy(c).start()

    def down(c, carry):
        out_copy(c).wait()
        part = jnp.dot(act[...], oring[lax.rem(c, OUT_SLOTS)], preferred_element_type=F32)

        @pl.when(c + OUT_SLOTS < chunks)
        def _():
            out_copy(c + OUT_SLOTS).start(priority=1)

        send_d[c] = part[2 * rows:].astype(BF16)
        keep[lax.rem(c, 2)] = part[:2 * rows]
        die_copy(c).start()

        @pl.when(c > 0)
        def _():
            finish(c - 1)

        return carry

    lax.fori_loop(0, chunks, down, 0)
    finish(chunks - 1)
    for c in range(chunks):
        cols = pl.ds(c * OUT_COLS, OUT_COLS)
        chip_copy(c).wait_recv()
        y_ref[:, cols] = (hid[:, cols] + recv_i[c].astype(F32)).astype(BF16)
    for copy in (*to_cross, to_partner, *forward):
        copy.wait_send()
    for c in range(chunks):
        die_copy(c).wait_send()
        chip_copy(c).wait_send()


def solution(mesh):
    row_spec = P(('rep', 'grp'))
    repl_spec = P()
    vmem = pl.BlockSpec(memory_space=pltpu.VMEM)
    hbm = pl.BlockSpec(memory_space=pl.ANY)
    dma = pltpu.SemaphoreType.DMA

    def local_layer(x_in, seq_len, k_cache, v_cache, gamma_attn, w_qkv, b_qkv, w_proj, gamma_mlp, w_in, w_out):
        rows, width = x_in.shape
        cache_len, kv_heads = k_cache.shape[1:3]
        q_heads = w_proj.shape[0] // HEAD
        ffn = w_out.shape[0]
        cache_rows = cache_len * kv_heads

        flat = jax.ShapeDtypeStruct((rows, cache_rows, HEAD), BF16)
        mlp_in, hidden, k_out, v_out = pl.pallas_call(
            functools.partial(attention_kernel, q_heads, kv_heads),
            out_shape=(jax.ShapeDtypeStruct((rows, width), BF16), jax.ShapeDtypeStruct((rows, width), F32), flat, flat),
            in_specs=[hbm] * 9,
            out_specs=(vmem, vmem, hbm, hbm),
            scratch_shapes=[
                pltpu.SMEM((rows,), jnp.int32),
                pltpu.VMEM((rows, width), BF16),
                pltpu.VMEM((width,), BF16),
                pltpu.VMEM((b_qkv.shape[0],), BF16),
                pltpu.VMEM((width,), BF16),
                pltpu.VMEM((QKV_SLOTS, width, QKV_COLS), BF16),
                pltpu.VMEM((SEQ_SLOTS, SEQ_STEP, cache_rows, HEAD), BF16),
                pltpu.VMEM((SEQ_SLOTS, SEQ_STEP, cache_rows, HEAD), BF16),
                pltpu.VMEM((rows, HEAD), F32),
                pltpu.VMEM((rows, width), BF16),
                pltpu.VMEM((rows, HEAD_ROWS, HEAD), F32),
                pltpu.VMEM((rows, 8, HEAD), F32),
                pltpu.VMEM((rows, 8, HEAD), F32),
                pltpu.VMEM((rows, HEAD_ROWS, HEAD), F32),
                dma((5,)), dma((QKV_SLOTS,)), dma((SEQ_SLOTS,)), dma((SEQ_SLOTS,)), dma((SEQ_SLOTS,)), dma((SEQ_SLOTS,)),
            ],
            compiler_params=pltpu.CompilerParams(vmem_limit_bytes=60 * 1024 * 1024),
            name="attention",
        )(seq_len, x_in, gamma_attn, b_qkv, gamma_mlp, w_qkv, w_proj,
          k_cache.reshape(rows, cache_rows, HEAD), v_cache.reshape(rows, cache_rows, HEAD))

        chunks = width // OUT_COLS
        layer_out = pl.pallas_call(
            mlp_kernel,
            out_shape=jax.ShapeDtypeStruct((rows, width), BF16),
            in_specs=[hbm] * 4,
            out_specs=vmem,
            scratch_shapes=[
                pltpu.VMEM((FF_SLOTS, 2, FF_BLOCK, width), BF16),
                pltpu.VMEM((FF_BLOCK, width), BF16),
                pltpu.VMEM((OUT_SLOTS, ffn, OUT_COLS), BF16),
                pltpu.VMEM((4 * rows, width), BF16),
                pltpu.VMEM((rows, width), F32),
                pltpu.VMEM((4 * rows, ffn), BF16),
                pltpu.VMEM((chunks, 2 * rows, OUT_COLS), BF16),
                pltpu.VMEM((chunks, 2 * rows, OUT_COLS), BF16),
                pltpu.VMEM((2, 2 * rows, OUT_COLS), F32),
                pltpu.VMEM((chunks, rows, OUT_COLS), BF16),
                pltpu.VMEM((chunks, rows, OUT_COLS), BF16),
                dma, dma, dma((FF_SLOTS,)), dma((2,)), dma((OUT_SLOTS,)),
                dma((AG_CHUNKS,)), dma((AG_CHUNKS,)), dma, dma, dma((AG_CHUNKS,)), dma((AG_CHUNKS,)),
                dma((chunks,)), dma((chunks,)), dma((chunks,)), dma((chunks,)),
            ],
            compiler_params=pltpu.CompilerParams(collective_id=0, has_side_effects=True,
                                                 vmem_limit_bytes=67043328),
            name="mlp",
        )(mlp_in, hidden, w_in, w_out)
        return layer_out, k_out.reshape(k_cache.shape), v_out.reshape(v_cache.shape)

    return jax.shard_map(local_layer, mesh=mesh,
                         in_specs=(row_spec, row_spec, row_spec, row_spec, repl_spec, repl_spec, repl_spec,
                                   repl_spec, repl_spec, P(None, 'grp', None), P('grp', None)),
                         out_specs=(row_spec, row_spec, row_spec), check_vma=False)
```
